32 devices in a mesh: dp: 4 (over x, core), ctx: 4 (over z), tensor: 2 (over y).
Axes of the slice: x: 2, y: 2, z: 4, core: 2. Of those that a mesh axis runs over, the one named last changes fastest.
Arguments:
- block_in: bfloat16 [8, 512, 2048], P('dp', 'ctx'), may hold values from -8 to 8
- attn_gain: bfloat16 [2048], replicated, may hold values from 0.5 to 1.5
- query_weight: bfloat16 [2048, 2048], P(None, 'tensor'), may hold values from -1 to 1
- key_weight: bfloat16 [2048, 512], P(None, 'tensor'), may hold values from -1 to 1
- value_weight: bfloat16 [2048, 512], P(None, 'tensor'), may hold values from -0.125 to 0.125
- output_weight: bfloat16 [2048, 2048], P('tensor'), may hold values from -0.75 to 0.75
- mlp_gain: bfloat16 [2048], replicated, may hold values from 0.5 to 1.5
- gate_weight: bfloat16 [2048, 8192], P(None, 'tensor'), may hold values from -0.125 to 0.125
- up_weight: bfloat16 [2048, 8192], P(None, 'tensor'), may hold values from -0.125 to 0.125
- down_weight: bfloat16 [8192, 2048], P('tensor'), may hold values from -0.0625 to 0.0625
- cotangent: bfloat16 [8, 512, 2048], P('dp', 'ctx'), may hold values from -6 to 6
Outputs:
- block_out: bfloat16 [8, 512, 2048], P('dp', ('ctx', 'tensor'))
- input_grad: float32 [8, 512, 2048], P('dp', ('ctx', 'tensor'))
- grad_attn_gain: float32 [2048], P(('dp', 'ctx'))
- grad_query: float32 [2048, 2048], P(('dp', 'ctx'), 'tensor')
- grad_key: float32 [2048, 512], P(('dp', 'ctx'), 'tensor')
- grad_value: float32 [2048, 512], P(('dp', 'ctx'), 'tensor')
- grad_output: float32 [2048, 2048], P('tensor', ('dp', 'ctx'))
- grad_mlp_gain: float32 [2048], P(('dp', 'ctx'))
- grad_gate: float32 [2048, 8192], P(('dp', 'ctx'), 'tensor')
- grad_up: float32 [2048, 8192], P(('dp', 'ctx'), 'tensor')
- grad_down: float32 [8192, 2048], P('tensor', ('dp', 'ctx'))
The draws below stay inside these ranges and needn't reach their ends.
All inputs are finite; a program needn't handle non-finite values.
Results may differ from the reference program's by a relative error of at most 0.024.
Values may be sent and summed in bfloat16 or wider, within the bound.
A program may use at most 256 MiB of HBM per device.

```python
import jax
import jax.numpy as jnp
from jax import lax

D = 2048
HEADS = 32
KV_HEADS = 8
HD = 64
FF = 8192
BATCH = 8
SEQ = 512


def draw_block_in(key, part):
    drawn = jax.random.normal(jax.random.fold_in(key, 11), (BATCH, SEQ, D), jnp.float32)
    return jnp.clip(drawn, -8.0, 8.0).astype(jnp.bfloat16)


def drawn_weight(key, salt, head_count):
    columns = head_count * HD
    drawn = jax.random.normal(jax.random.fold_in(key, salt), (D, columns), jnp.float32)
    return jnp.clip(drawn * D ** (-0.5), -1.0, 1.0).astype(jnp.bfloat16)


def draw_query_weight(key, part):
    return drawn_weight(key, 21, HEADS)


def draw_key_weight(key, part):
    return drawn_weight(key, 31, KV_HEADS)


def levels(rng, dims, shards, least, high):
    def one(axis_at, shards_of):
        steps = jax.random.uniform(jax.random.fold_in(jax.random.fold_in(rng, 6), axis_at), (shards_of,), jnp.float32, least / len(shards), high / len(shards))
        return jnp.repeat(jnp.exp(steps), dims[axis_at] // shards_of).reshape((-1,) + (1,) * (len(dims) - axis_at - 1))

    factor_of = one(*shards[0])
    for cut in shards[1:]:
        factor_of = factor_of * one(*cut)
    return factor_of


def scatter_about(key, dims, width, reach, pieces=(), kind=jnp.bfloat16):
    values = jax.random.normal(key, dims, jnp.float32) * width
    if len(pieces) > 0:
        values = levels(key, dims, pieces, -0.22, 0.18) * values
    return jnp.clip(values, min=-reach, max=reach).astype(kind)


def setup_inputs(seed: int = 0) -> dict:
    streams_of = jax.random.split(jax.random.key(seed), 12)
    block_in = draw_block_in(jax.random.fold_in(streams_of[11], 71), 0)
    attn_gain = jnp.clip(1.0 + 0.1 * jax.random.normal(streams_of[1], (D,), jnp.float32), 0.5, 1.5).astype(jnp.bfloat16)
    query_weight = draw_query_weight(jax.random.fold_in(streams_of[11], 71), 0)
    key_weight = draw_key_weight(jax.random.fold_in(streams_of[11], 71), 0)
    value_weight = scatter_about(streams_of[4], (D, KV_HEADS * HD), D ** -0.5, 0.125, ((1, 2),))
    output_weight = scatter_about(streams_of[5], (HEADS * HD, D), HD ** -0.5, 0.75, ((0, 2),))
    mlp_gain = jnp.clip(1.0 + 0.1 * jax.random.normal(streams_of[6], (D,), jnp.float32), 0.5, 1.5).astype(jnp.bfloat16)
    gate_weight = scatter_about(streams_of[7], (D, FF), D ** -0.5, 0.125, ((1, 2),))
    up_weight = scatter_about(streams_of[8], (D, FF), D ** -0.5, 0.125, ((1, 2),))
    down_weight = scatter_about(streams_of[9], (FF, D), FF ** -0.5, 0.0625, ((0, 2),))
    cotangent = scatter_about(streams_of[10], (BATCH, SEQ, D), 1.0, 6.0, ((0, 4), (1, 4)))
    return dict(block_in=block_in, attn_gain=attn_gain, query_weight=query_weight, key_weight=key_weight, value_weight=value_weight, output_weight=output_weight, mlp_gain=mlp_gain, gate_weight=gate_weight, up_weight=up_weight, down_weight=down_weight, cotangent=cotangent)


@jax.custom_vjp
def low(v):
    return lax.optimization_barrier(v.astype(jnp.bfloat16)).astype(jnp.float32)

@jax.custom_vjp
def low_back(v):
    return v

def low_keep(v):
    return (low(v), None)

def low_pass(kept, grad):
    return (grad,)

def back_keep(v):
    return (v, None)

def back_low(kept, grad):
    return (low(grad),)
low.defvjp(low_keep, low_pass)
low_back.defvjp(back_keep, back_low)
norm_eps = 1e-05
rope_base = 500000.0
highest = lax.Precision.HIGHEST

def rope_tables(length):
    half_width = HD // 2
    frequency = rope_base ** (-jnp.arange(half_width, dtype=jnp.float32) * 2.0 / HD)
    angles = jnp.arange(length, dtype=jnp.float32)[:, None] * frequency[None, :]
    return (jnp.cos(angles)[:, None, :], jnp.sin(angles)[:, None, :])

def rotate(vectors, cosine, sine_table):
    half_width = vectors.shape[-1] // 2
    first_half = vectors[..., :half_width]
    second_half = vectors[..., half_width:]
    return jnp.concatenate([first_half * cosine - second_half * sine_table, second_half * cosine + first_half * sine_table], axis=-1)

def rms_apply(values, gain):
    return values * lax.rsqrt(lax.optimization_barrier(jnp.mean(values * values, axis=-1, keepdims=True)) + norm_eps) * gain

def layer(block_in, attn_gain, query_weight, key_weight, value_weight, output_weight, mlp_gain, gate_weight, up_weight, down_weight):
    length = block_in.shape[0]
    normed = low(rms_apply(block_in, attn_gain))
    query_raw = jnp.dot(normed, query_weight, precision=highest).reshape(length, HEADS, HD)
    key_raw = jnp.dot(normed, key_weight, precision=highest).reshape(length, KV_HEADS, HD)
    value_raw = jnp.dot(normed, value_weight, precision=highest).reshape(length, KV_HEADS, HD)
    cosine, sine_table = rope_tables(length)
    queries = low(rotate(low_back(query_raw), cosine, sine_table))
    keys = low(rotate(low_back(key_raw), cosine, sine_table))
    values = low(low_back(value_raw))
    group_size = HEADS // KV_HEADS
    keys = jnp.repeat(keys, group_size, axis=1)
    values = jnp.repeat(values, group_size, axis=1)
    scores = low_back(jnp.einsum('qhd,khd->hqk', queries, keys, precision=highest) * HD ** (-0.5))
    positions = jnp.arange(length)
    causal = positions[:, None] >= positions[None, :]
    masked = jnp.where(causal[None], scores, -1e+30)
    attn_probs = low(jax.nn.softmax(masked, axis=-1))
    attended = jnp.einsum('hqk,khd->qhd', attn_probs, values, precision=highest)
    attended = low(low_back(attended)).reshape(length, HEADS * HD)
    hidden = block_in + low_back(jnp.dot(attended, output_weight, precision=highest))
    normed_mlp = low(rms_apply(hidden, mlp_gain))
    gate_val = low_back(jnp.dot(normed_mlp, gate_weight, precision=highest))
    up_val = low_back(jnp.dot(normed_mlp, up_weight, precision=highest))
    activated = low(jax.nn.silu(gate_val) * up_val)
    return hidden + jnp.dot(activated, down_weight, precision=highest)

def reference(block_in, attn_gain, query_weight, key_weight, value_weight, output_weight, mlp_gain, gate_weight, up_weight, down_weight, cotangent):
    params = tuple((member.astype(jnp.float32) for member in (attn_gain, query_weight, key_weight, value_weight, output_weight, mlp_gain, gate_weight, up_weight, down_weight)))

    def one_sequence(running, seq_pair):
        seq_input, seq_cotangent = seq_pair
        outputs, pull_back = jax.vjp(layer, seq_input.astype(jnp.float32), *params)
        grad_list = pull_back(seq_cotangent.astype(jnp.float32))
        running = tuple((summed + new_grad for summed, new_grad in zip(running, grad_list[1:])))
        return (running, (outputs.astype(jnp.bfloat16), grad_list[0]))
    zero_grads = tuple((jnp.zeros(member.shape, jnp.float32) for member in params))
    totals, (block_out, input_grad) = lax.scan(one_sequence, zero_grads, (block_in, cotangent))
    return (block_out, input_grad, totals[0], totals[1], totals[2], totals[3], totals[4], totals[5], totals[6], totals[7], totals[8])
```

```python
import jax
import jax.numpy as jnp
from jax import lax
from jax.sharding import PartitionSpec as P

HD = 64

norm_eps = 1e-05
rope_base = 500000.0
f32 = jnp.float32
bf16 = jnp.bfloat16


def rms_apply(values, gain):
    return values * lax.rsqrt(jnp.mean(values * values, axis=-1, keepdims=True) + norm_eps) * gain


def rope_tables(positions, head_size):
    half_width = head_size // 2
    frequency = rope_base ** (-jnp.arange(half_width, dtype=f32) * 2.0 / head_size)
    angles = positions.astype(f32)[:, None] * frequency[None, :]
    return (jnp.cos(angles)[:, None, :], jnp.sin(angles)[:, None, :])


def rotate(vectors, cosine, sine_table):
    half_width = vectors.shape[-1] // 2
    first_half = vectors[..., :half_width]
    second_half = vectors[..., half_width:]
    return jnp.concatenate(
        [
            first_half * cosine - second_half * sine_table,
            second_half * cosine + first_half * sine_table,
        ],
        axis=-1,
    )


def dot_nn(left, right):
    return lax.dot_general(left, right, (((1,), (0,)), ((), ())), preferred_element_type=f32)


def dot_tn(left, right):
    return lax.dot_general(left, right, (((0,), (0,)), ((), ())), preferred_element_type=f32)


def dot_nt(left, right):
    return lax.dot_general(left, right, (((1,), (1,)), ((), ())), preferred_element_type=f32)


def xor_pairs(count, bit):
    return [(i, i ^ bit) for i in range(count)]


def dp_bits():
    count = lax.axis_size("dp")
    bits = []
    bit = count // 2
    while bit:
        bits.append(bit)
        bit //= 2
    return count, bits


def dp_rows(rows):
    count, bits = dp_bits()
    for bit in bits:
        rows = jnp.concatenate([rows, lax.ppermute(rows, "dp", xor_pairs(count, bit))], axis=0)
    return rows


def dp_columns(rows):
    count, bits = dp_bits()
    me = lax.axis_index("dp")
    for bit in bits:
        half = rows.shape[1] // 2
        upper = (me // bit) % 2
        keep = lax.dynamic_slice_in_dim(rows, upper * half, half, 1)
        give = lax.dynamic_slice_in_dim(rows, (1 - upper) * half, half, 1)
        rows = jnp.concatenate([keep, lax.ppermute(give, "dp", xor_pairs(count, bit))], axis=0)
    return rows


def swap_tensor(values):
    return lax.ppermute(values, "tensor", [(0, 1), (1, 0)])


def sum_share(part):
    ranks = lax.axis_size("tensor")
    if ranks != 2:
        return lax.psum_scatter(part.astype(bf16), "tensor", scatter_dimension=1, tiled=True).astype(f32)
    share = part.shape[1] // 2
    me = lax.axis_index("tensor")
    mine = lax.dynamic_slice_in_dim(part, me * share, share, 1)
    theirs = lax.dynamic_slice_in_dim(part, (1 - me) * share, share, 1)
    return mine + swap_tensor(theirs.astype(bf16)).astype(f32)


def sum_whole(part):
    if lax.axis_size("tensor") != 2:
        return lax.psum(part.astype(bf16), "tensor").astype(f32)
    low = part.astype(bf16)
    return low.astype(f32) + swap_tensor(low).astype(f32)


def other_weight(weight):
    count, _ = dp_bits()
    half = weight.shape[0] // 2
    parity = lax.axis_index("dp") % 2
    got = swap_tensor(lax.dynamic_slice_in_dim(weight, parity * half, half, 0))
    also = lax.ppermute(got, "dp", xor_pairs(count, 1))
    even = parity == 0
    return jnp.concatenate([jnp.where(even, got, also), jnp.where(even, also, got)], axis=0)


def ctx_scatter(block):
    return lax.psum_scatter(block.astype(bf16), "ctx", scatter_dimension=0, tiled=True).astype(f32)


def shards(
    block_in,
    attn_gain,
    query_weight,
    key_weight,
    value_weight,
    output_weight,
    mlp_gain,
    gate_weight,
    up_weight,
    down_weight,
    cotangent,
):
    seq_count, ctx_tok, width = block_in.shape
    ctx_ranks = lax.axis_size("ctx")
    tensor_ranks = lax.axis_size("tensor")
    share_len = ctx_tok // tensor_ranks
    share_start = lax.axis_index("tensor") * share_len
    rows = seq_count * ctx_tok
    query_heads = query_weight.shape[1] // HD
    key_heads = key_weight.shape[1] // HD
    kv_cols = key_heads * HD
    group = query_heads // key_heads
    scale = HD ** (-0.5)
    ctx_at = lax.axis_index("ctx")

    def share_of(values):
        return lax.dynamic_slice_in_dim(values, share_start, share_len, 1)

    gain_first = attn_gain.astype(f32)
    gain_second = mlp_gain.astype(f32)
    input_full = block_in.astype(f32)
    cot_rows = cotangent.reshape(rows, width)
    r_first = lax.rsqrt(jnp.mean(input_full * input_full, axis=-1, keepdims=True) + norm_eps)
    unit_first = input_full * r_first
    normed = (unit_first * gain_first).astype(bf16).reshape(rows, width)

    key_raw = dot_nn(normed, key_weight).reshape(seq_count, ctx_tok, key_heads, HD)
    value_raw = dot_nn(normed, value_weight)
    positions = ctx_at * ctx_tok + jnp.arange(ctx_tok, dtype=jnp.int32)
    cosine, sine = rope_tables(positions, HD)
    keys_local = rotate(key_raw, cosine, sine).astype(bf16).reshape(seq_count, ctx_tok, kv_cols)
    kv_local = jnp.concatenate(
        [keys_local, value_raw.astype(bf16).reshape(seq_count, ctx_tok, kv_cols)], axis=-1
    )
    blocks = [kv_local]
    for back in range(1, ctx_ranks):
        blocks.append(
            lax.ppermute(kv_local, "ctx", [(i, i + back) for i in range(ctx_ranks - back)])
        )
    kv_all = jnp.concatenate(blocks, axis=1)
    seq_len = kv_all.shape[1]
    keys_all = kv_all[..., :kv_cols].reshape(seq_count, seq_len, key_heads, HD)
    values_all = kv_all[..., kv_cols:].reshape(seq_count, seq_len, key_heads, HD)
    query_raw = dot_nn(normed, query_weight).reshape(seq_count, ctx_tok, query_heads, HD)
    queries = (
        rotate(query_raw, cosine, sine)
        .astype(bf16)
        .reshape(seq_count, ctx_tok, key_heads, group, HD)
    )
    key_at = jnp.arange(seq_len, dtype=jnp.int32)
    key_back = key_at // ctx_tok
    query_at = jnp.arange(ctx_tok, dtype=jnp.int32)
    causal = jnp.where(
        key_back[None, :] == 0,
        query_at[:, None] >= key_at[None, :],
        (key_back <= ctx_at)[None, :],
    )

    def scored(query_seq, key_seq):
        raw = jnp.einsum("qkgd,skd->kgqs", query_seq, key_seq, preferred_element_type=f32) * scale
        return jnp.where(causal, raw, -1e30)

    def forward_one(seq_parts):
        query_seq, key_seq, value_seq = seq_parts
        masked = scored(query_seq, key_seq)
        row_max = jnp.max(masked, axis=-1, keepdims=True)
        unnormed = jnp.exp(masked - row_max)
        row_total = jnp.sum(unnormed, axis=-1, keepdims=True)
        probs_low = (unnormed / row_total).astype(bf16)
        attended_seq = jnp.einsum("kgqs,skd->qkgd", probs_low, value_seq, preferred_element_type=f32)
        return (attended_seq.astype(bf16), row_max, row_total)

    attended, row_maxes, row_totals = lax.map(forward_one, (queries, keys_all, values_all))
    attended_flat = attended.reshape(rows, query_heads * HD)
    branch = dot_nn(attended_flat, output_weight)
    if tensor_ranks == 2:
        branch = branch + dot_nn(swap_tensor(attended_flat), other_weight(output_weight))
    else:
        branch = lax.psum(branch, "tensor")
    hidden = input_full + branch.reshape(seq_count, ctx_tok, width)
    r_second = lax.rsqrt(jnp.mean(hidden * hidden, axis=-1, keepdims=True) + norm_eps)
    unit_second = hidden * r_second
    normed_mlp = (unit_second * gain_second).astype(bf16).reshape(rows, width)

    grad_activated = dot_nt(cot_rows, down_weight)
    gate_val = dot_nn(normed_mlp, gate_weight)
    up_val = dot_nn(normed_mlp, up_weight)
    sig = jax.nn.sigmoid(gate_val)
    silu = gate_val * sig
    activated = (silu * up_val).astype(bf16)
    grad_gate_val = (grad_activated * up_val * sig * (1.0 + gate_val * (1.0 - sig))).astype(bf16)
    grad_up_val = (grad_activated * silu).astype(bf16)
    mlp_part = dot_nn(activated, down_weight).reshape(seq_count, ctx_tok, width)
    grad_normed_part = (
        dot_nt(grad_gate_val, gate_weight) + dot_nt(grad_up_val, up_weight)
    ).reshape(seq_count, ctx_tok, width)
    mlp_gain_part = jnp.sum(grad_normed_part * unit_second, axis=(0, 1))

    act_all = dp_rows(activated)
    cot_cols = dp_columns(cot_rows)
    grad_down = ctx_scatter(dot_tn(cot_cols, act_all)).T
    nm_cols = dp_columns(normed_mlp)
    grad_gate = ctx_scatter(dot_tn(nm_cols, dp_rows(grad_gate_val)))
    grad_up = ctx_scatter(dot_tn(nm_cols, dp_rows(grad_up_val)))

    block_out = (share_of(hidden) + sum_share(mlp_part)).astype(bf16)
    grad_normed = sum_whole(grad_normed_part)
    scaled = gain_second * grad_normed
    grad_hidden = cotangent.astype(f32) + r_second * (
        scaled - unit_second * jnp.mean(scaled * unit_second, axis=-1, keepdims=True)
    )
    grad_branch = grad_hidden.astype(bf16).reshape(rows, width)
    grad_attended = (
        dot_nt(grad_branch, output_weight)
        .astype(bf16)
        .reshape(seq_count, ctx_tok, key_heads, group, HD)
    )
    grad_output = ctx_scatter(dot_tn(dp_columns(grad_branch), dp_rows(attended_flat))).T

    def backward_one(seq_parts):
        query_seq, key_seq, value_seq, grad_seq, row_max, row_total = seq_parts
        masked = scored(query_seq, key_seq)
        attn_probs = jnp.exp(masked - row_max) / row_total
        probs_low = attn_probs.astype(bf16)
        grad_probs = jnp.einsum("qkgd,skd->kgqs", grad_seq, value_seq, preferred_element_type=f32)
        inner_sum = jnp.sum(attn_probs * grad_probs, axis=-1, keepdims=True)
        grad_scores = (attn_probs * (grad_probs - inner_sum)).astype(bf16)
        grad_query_seq = (
            jnp.einsum("kgqs,skd->qkgd", grad_scores, key_seq, preferred_element_type=f32) * scale
        )
        grad_key_seq = (
            jnp.einsum("kgqs,qkgd->skd", grad_scores, query_seq, preferred_element_type=f32) * scale
        )
        grad_value_seq = jnp.einsum("kgqs,qkgd->skd", probs_low, grad_seq, preferred_element_type=f32)
        return (grad_query_seq, grad_key_seq, grad_value_seq)

    grad_queries, grad_keys, grad_values = lax.map(
        backward_one, (queries, keys_all, values_all, grad_attended, row_maxes, row_totals)
    )
    grad_kv = jnp.concatenate(
        [
            grad_keys.reshape(seq_count, seq_len, kv_cols),
            grad_values.reshape(seq_count, seq_len, kv_cols),
        ],
        axis=-1,
    )
    kv_sum = grad_kv[:, :ctx_tok]
    for back in range(1, ctx_ranks):
        piece = grad_kv[:, back * ctx_tok : (back + 1) * ctx_tok].astype(bf16)
        kv_sum = kv_sum + lax.ppermute(
            piece, "ctx", [(i + back, i) for i in range(ctx_ranks - back)]
        ).astype(f32)
    grad_query_raw = (
        rotate(grad_queries.reshape(seq_count, ctx_tok, query_heads, HD), cosine, -sine)
        .astype(bf16)
        .reshape(rows, query_heads * HD)
    )
    grad_key_raw = (
        rotate(kv_sum[..., :kv_cols].reshape(seq_count, ctx_tok, key_heads, HD), cosine, -sine)
        .astype(bf16)
        .reshape(rows, kv_cols)
    )
    grad_value_raw = kv_sum[..., kv_cols:].astype(bf16).reshape(rows, kv_cols)
    normed_cols = dp_columns(normed)
    grad_query = ctx_scatter(dot_tn(normed_cols, dp_rows(grad_query_raw)))
    grad_key_value = ctx_scatter(
        dot_tn(normed_cols, dp_rows(jnp.concatenate([grad_key_raw, grad_value_raw], axis=-1)))
    )
    grad_key = grad_key_value[:, :kv_cols]
    grad_value = grad_key_value[:, kv_cols:]
    grad_normed_first = (
        dot_nt(grad_query_raw, query_weight)
        + dot_nt(grad_key_raw, key_weight)
        + dot_nt(grad_value_raw, value_weight)
    ).reshape(seq_count, ctx_tok, width)
    attn_gain_part = jnp.sum(grad_normed_first * unit_first, axis=(0, 1))
    gains = lax.psum(
        jnp.stack([attn_gain_part, mlp_gain_part]), ("dp", "ctx", "tensor")
    )
    gain_rows = width // (lax.axis_size("dp") * ctx_ranks)
    gain_at = (lax.axis_index("dp") * ctx_ranks + ctx_at) * gain_rows
    gains = lax.dynamic_slice_in_dim(gains, gain_at, gain_rows, 1)

    scaled_first = gain_first * sum_share(grad_normed_first)
    unit_share = share_of(unit_first)
    input_grad = share_of(grad_hidden) + share_of(r_first) * (
        scaled_first - unit_share * jnp.mean(scaled_first * unit_share, axis=-1, keepdims=True)
    )
    return (
        block_out,
        input_grad,
        gains[0],
        grad_query,
        grad_key,
        grad_value,
        grad_output,
        gains[1],
        grad_gate,
        grad_up,
        grad_down,
    )


def solution(mesh):
    in_specs = (
        P("dp", "ctx", None),
        P(),
        P(None, "tensor"),
        P(None, "tensor"),
        P(None, "tensor"),
        P("tensor", None),
        P(),
        P(None, "tensor"),
        P(None, "tensor"),
        P("tensor", None),
        P("dp", "ctx", None),
    )
    out_specs = (
        P("dp", ("ctx", "tensor"), None),
        P("dp", ("ctx", "tensor"), None),
        P(("dp", "ctx")),
        P(("dp", "ctx"), "tensor"),
        P(("dp", "ctx"), "tensor"),
        P(("dp", "ctx"), "tensor"),
        P("tensor", ("dp", "ctx")),
        P(("dp", "ctx")),
        P(("dp", "ctx"), "tensor"),
        P(("dp", "ctx"), "tensor"),
        P("tensor", ("dp", "ctx")),
    )
    return jax.shard_map(shards, mesh=mesh, in_specs=in_specs, out_specs=out_specs, check_vma=False)
```

```python
import jax
import jax.numpy as jnp
from jax import lax
from jax.experimental import pallas as pl
from jax.experimental.pallas import tpu as pltpu
from jax.sharding import PartitionSpec as P

HD = 64

norm_eps = 1e-05
rope_base = 500000.0
f32 = jnp.float32
bf16 = jnp.bfloat16


def rms_apply(values, gain):
    return values * lax.rsqrt(jnp.mean(values * values, axis=-1, keepdims=True) + norm_eps) * gain


def rope_tables(positions, head_size):
    half_width = head_size // 2
    frequency = rope_base ** (-jnp.arange(half_width, dtype=f32) * 2.0 / head_size)
    angles = positions.astype(f32)[:, None] * frequency[None, :]
    return (jnp.cos(angles)[:, None, :], jnp.sin(angles)[:, None, :])


def dot_nn(left, right):
    return lax.dot_general(left, right, (((1,), (0,)), ((), ())), preferred_element_type=f32)


def dot_tn(left, right):
    return lax.dot_general(left, right, (((0,), (0,)), ((), ())), preferred_element_type=f32)


def dot_nt(left, right):
    return lax.dot_general(left, right, (((1,), (1,)), ((), ())), preferred_element_type=f32)


def call(body, grid, in_specs, out_specs, out_shape, flops, moved, **rest):
    return pl.pallas_call(
        body,
        grid=grid,
        in_specs=in_specs,
        out_specs=out_specs,
        out_shape=out_shape,
        cost_estimate=pl.CostEstimate(flops=flops, bytes_accessed=moved, transcendentals=0),
        compiler_params=pltpu.CompilerParams(vmem_limit_bytes=56 << 20),
        **rest,
    )


def whole(shape):
    zeros = (0,) * len(shape)
    return pl.BlockSpec(shape, lambda *_: zeros, pipeline_mode=pl.Buffered(1))


def shape_of(shape, kind):
    return jax.ShapeDtypeStruct(shape, kind)


def turned(values, cosine, sine):
    at = lax.broadcasted_iota(jnp.int32, values.shape, 1) % HD
    swapped = jnp.where(
        at < HD // 2, pltpu.roll(values, 128 - HD // 2, 1), pltpu.roll(values, HD // 2, 1)
    )
    return values * cosine + swapped * sine


def rope_columns(positions):
    cosine, sine = rope_tables(positions, HD)
    cosine, sine = cosine[:, 0], sine[:, 0]
    return jnp.tile(cosine, (1, 4)), jnp.tile(jnp.concatenate([-sine, sine], axis=-1), (1, 2))


def norm_kv(rows, gain, key_weight, value_weight, cosine, sine):
    count, width = rows.shape
    cols = key_weight.shape[1]
    tokens = cosine.shape[0]

    def body(rows_ref, gain_ref, key_ref, value_ref, cos_ref, sin_ref, normed_ref, kv_ref):
        values = rows_ref[...].astype(f32)
        normed = rms_apply(values, gain_ref[...].astype(f32)).astype(bf16)
        normed_ref[...] = normed
        raw = jnp.concatenate([dot_nn(normed, key_ref[...]), dot_nn(normed, value_ref[...])], axis=1)
        for first in range(0, count, tokens):
            for at in range(0, 2 * cols, 128):
                part = raw[first : first + tokens, at : at + 128]
                kv_ref[first : first + tokens, at : at + 128] = turned(
                    part, cos_ref[:, at : at + 128], sin_ref[:, at : at + 128]
                ).astype(bf16)

    shapes = [rows.shape, gain.shape, key_weight.shape, value_weight.shape, cosine.shape, sine.shape]
    return call(
        body,
        (1,),
        [whole(s) for s in shapes],
        [whole(rows.shape), whole((count, 2 * cols))],
        [shape_of(rows.shape, bf16), shape_of((count, 2 * cols), bf16)],
        4 * count * width * cols,
        2 * (2 * count * width + 2 * width * cols),
    )(rows, gain, key_weight, value_weight, cosine, sine)


def tile_of(*sizes):
    for tile in (512, 256, 128):
        if all(size % tile == 0 for size in sizes):
            return tile
    raise ValueError("no tile")


def project_queries(normed, weight, cosine, sine):
    count, width = normed.shape
    cols = weight.shape[1]
    tokens = cosine.shape[0]
    tile = tile_of(cols)

    def body(normed_ref, weight_ref, cos_ref, sin_ref, out_ref):
        raw = dot_nn(normed_ref[...], weight_ref[...])
        for first in range(0, count, tokens):
            for at in range(0, tile, 128):
                out_ref[first : first + tokens, at : at + 128] = turned(
                    raw[first : first + tokens, at : at + 128], cos_ref[...], sin_ref[...]
                ).astype(bf16)

    return call(
        body,
        (cols // tile,),
        [
            whole(normed.shape),
            pl.BlockSpec((width, tile), lambda i: (0, i)),
            whole(cosine.shape),
            whole(sine.shape),
        ],
        pl.BlockSpec((count, tile), lambda i: (0, i)),
        shape_of((count, cols), bf16),
        2 * count * width * cols,
        2 * (count * width + width * cols),
    )(normed, weight, cosine, sine)


def scores_of(stacked, keys, ctx_at, scale):
    tokens = keys[0].shape[0]
    found = []
    for back, block in enumerate(keys):
        raw = dot_nt(stacked, block) * scale
        if back == 0:
            query_at = lax.broadcasted_iota(jnp.int32, raw.shape, 0) % tokens
            seen = query_at >= lax.broadcasted_iota(jnp.int32, raw.shape, 1)
            found.append(jnp.where(seen, raw, -1e30))
        else:
            found.append(raw + jnp.where(ctx_at >= back, 0.0, -1e30).astype(f32))
    most = jnp.max(found[0], axis=-1, keepdims=True)
    for masked in found[1:]:
        most = jnp.maximum(most, jnp.max(masked, axis=-1, keepdims=True))
    found = [jnp.exp(masked - most) for masked in found]
    total = sum(jnp.sum(part, axis=-1, keepdims=True) for part in found)
    inverse = 1.0 / total
    return [part * inverse for part in found]


def stack_heads(ref, head, group):
    first = head * group
    return jnp.concatenate(
        [ref[:, (first + g) * HD : (first + g + 1) * HD] for g in range(group)], axis=0
    )


def attend(queries, kv_blocks, tokens):
    count, cols = queries.shape
    kv_cols = kv_blocks[0].shape[1] // 2
    heads = kv_cols // HD
    group = cols // kv_cols
    scale = HD ** (-0.5)
    blocks = len(kv_blocks)

    def body(query_ref, *refs):
        out_ref = refs[-1]
        ctx_at = lax.axis_index("ctx")
        for head in range(heads):
            stacked = stack_heads(query_ref, head, group)
            at = head * HD
            keys = [ref[:, at : at + HD] for ref in refs[:blocks]]
            probs = scores_of(stacked, keys, ctx_at, scale)
            total = sum(
                dot_nn(part.astype(bf16), ref[:, kv_cols + at : kv_cols + at + HD])
                for part, ref in zip(probs, refs)
            )
            for g in range(group):
                first = (head * group + g) * HD
                out_ref[:, first : first + HD] = total[g * tokens : (g + 1) * tokens].astype(bf16)

    rows = lambda width: pl.BlockSpec((tokens, width), lambda i: (i, 0))
    return call(
        body,
        (count // tokens,),
        [rows(cols)] + [rows(2 * kv_cols)] * blocks,
        rows(cols),
        shape_of((count, cols), bf16),
        40 * count * cols * tokens * blocks,
        2 * count * (2 * cols + 2 * kv_cols * blocks),
    )(queries, *kv_blocks)


def attend_back(queries, kv_blocks, grad_attended, cosine, sine, tokens):
    count, cols = queries.shape
    kv_cols = kv_blocks[0].shape[1] // 2
    heads = kv_cols // HD
    group = cols // kv_cols
    scale = HD ** (-0.5)
    blocks = len(kv_blocks)

    def body(query_ref, grad_ref, cos_ref, sin_ref, *refs):
        kv_refs, query_out, kv_out = refs[:blocks], refs[blocks], refs[blocks + 1 : -1]
        turned_ref = refs[-1]
        ctx_at = lax.axis_index("ctx")
        for head in range(heads):
            stacked = stack_heads(query_ref, head, group)
            grads = stack_heads(grad_ref, head, group)
            at = head * HD
            keys = [ref[:, at : at + HD] for ref in kv_refs]
            values = [ref[:, kv_cols + at : kv_cols + at + HD] for ref in kv_refs]
            probs = scores_of(stacked, keys, ctx_at, scale)
            grad_probs = [dot_nt(grads, block) for block in values]
            inner = sum(
                jnp.sum(part * grad, axis=-1, keepdims=True)
                for part, grad in zip(probs, grad_probs)
            )
            total = 0.0
            for back in range(blocks):
                grad_scores = (probs[back] * (grad_probs[back] - inner)).astype(bf16)
                total = total + dot_nn(grad_scores, keys[back])
                kind = kv_out[back].dtype
                kv_out[back][:, at : at + HD] = (dot_tn(grad_scores, stacked) * scale).astype(kind)
                kv_out[back][:, kv_cols + at : kv_cols + at + HD] = dot_tn(
                    probs[back].astype(bf16), grads
                ).astype(kind)
            for g in range(group):
                first = (head * group + g) * HD
                turned_ref[:, first : first + HD] = total[g * tokens : (g + 1) * tokens] * scale
        for at in range(0, cols, 128):
            query_out[:, at : at + 128] = turned(
                turned_ref[:, at : at + 128], cos_ref[...], -sin_ref[...]
            ).astype(bf16)

    rows = lambda width: pl.BlockSpec((tokens, width), lambda i: (i, 0))
    return call(
        body,
        (count // tokens,),
        [rows(cols), rows(cols), whole(cosine.shape), whole(sine.shape)]
        + [rows(2 * kv_cols)] * blocks,
        [rows(cols)] + [rows(2 * kv_cols)] * blocks,
        [shape_of((count, cols), bf16)]
        + [shape_of((count, 2 * kv_cols), f32 if back == 0 else bf16) for back in range(blocks)],
        100 * count * cols * tokens * blocks,
        2 * count * (3 * cols + 4 * kv_cols * blocks),
        scratch_shapes=[pltpu.VMEM((tokens, cols), f32)],
    )(queries, grad_attended, cosine, sine, *kv_blocks)


def mlp(normed, cot, gate_weight, up_weight, down_weight, start, size, sums, parts):
    count, width = normed.shape
    tile = tile_of(start, size)
    base = start // tile
    given = 0 if sums is None else 2

    def body(normed_ref, cot_ref, gate_ref, up_ref, down_ref, *refs):
        out_refs, down_sum, back_sum = refs[given:-2], refs[-2], refs[-1]
        first = pl.program_id(0) == 0
        gate = dot_nn(normed_ref[...], gate_ref[...])
        up = dot_nn(normed_ref[...], up_ref[...])
        grad = dot_nt(cot_ref[...], down_ref[...])
        sig = 1.0 / (1.0 + jnp.exp(-gate))
        silu = gate * sig
        activated = (silu * up).astype(bf16)
        grad_gate = (grad * up * sig * (1.0 + gate * (1.0 - sig))).astype(bf16)
        grad_up = (grad * silu).astype(bf16)
        made = [activated, grad_gate, grad_up]
        at = 0
        for ref in out_refs:
            for i in range(ref.shape[0]):
                ref[i] = made[at]
                at += 1

        @pl.when(first)
        def _():
            if given:
                down_sum[...] = refs[0][...]
                back_sum[...] = refs[1][...]
            else:
                down_sum[...] = jnp.zeros_like(down_sum)
                back_sum[...] = jnp.zeros_like(back_sum)

        down_sum[...] += dot_nn(activated, down_ref[...])
        back_sum[...] += dot_nt(grad_gate, gate_ref[...]) + dot_nt(grad_up, up_ref[...])

    held = whole((count, width))
    columns = pl.BlockSpec((width, tile), lambda i: (0, base + i))
    return call(
        body,
        (size // tile,),
        [held, held, columns, columns, pl.BlockSpec((tile, width), lambda i: (base + i, 0))]
        + [held] * given,
        [pl.BlockSpec((n, count, tile), lambda i: (0, 0, i)) for n in parts] + [held, held],
        [shape_of((n, count, size), bf16) for n in parts]
        + [shape_of((count, width), f32)] * 2,
        12 * count * width * size,
        2 * (3 * width * size + 3 * count * size + 10 * count * width),
        input_output_aliases={5: len(parts), 6: len(parts) + 1} if given else {},
    )(normed, cot, gate_weight, up_weight, down_weight, *(sums or ()))


def weight_grad(buffer, total, start, lefts, chosen, rights):
    entries, count, size = rights[0].shape
    own = lefts[0][0].shape[1]
    tile = tile_of(start, size)
    base, steps = start // tile, size // tile
    sources = len(rights)
    given = 0 if buffer is None else 1

    def body(*refs):
        out_ref = refs[-1]
        rights_at = refs[given + sources * len(lefts) : -1]

        def product(which):
            left = refs[given + sources * which : given + sources * (which + 1)]
            out_ref[...] = sum(dot_tn(a[...], b[0]) for a, b in zip(left, rights_at)).astype(bf16)

        for which in range(len(lefts)):
            if len(lefts) == 1:
                product(0)
            else:
                mine = [v for v in range(entries) if chosen[v] == which]
                v = pl.program_id(0)
                pl.when((v >= mine[0]) & (v <= mine[-1]))(lambda which=which: product(which))

    return call(
        body,
        (entries, steps),
        [pl.BlockSpec(memory_space=pl.ANY)] * given
        + [whole((count, own))] * (sources * len(lefts))
        + [pl.BlockSpec((1, count, tile), lambda v, i: (v, 0, i))] * sources,
        pl.BlockSpec((own, tile), lambda v, i: (0, base + v * steps + i)),
        shape_of((own, total), bf16),
        2 * entries * sources * count * own * size,
        2 * entries * size * (sources * count + own),
        input_output_aliases={0: 0} if given else {},
    )(*([] if buffer is None else [buffer]), *(p for left in lefts for p in left), *rights)


def xor_pairs(count, bit):
    return [(i, i ^ bit) for i in range(count)]


def dp_bits():
    count = lax.axis_size("dp")
    bits = []
    bit = count // 2
    while bit:
        bits.append(bit)
        bit //= 2
    return count, bits


def dp_rows(rows):
    count, bits = dp_bits()
    found = [rows]
    for bit in bits:
        found = found + [lax.ppermute(part, "dp", xor_pairs(count, bit)) for part in found]
    return found


def dp_columns(rows):
    count, bits = dp_bits()
    me = lax.axis_index("dp")
    found = [rows]
    for bit in bits:
        half = found[0].shape[1] // 2
        upper = (me // bit) % 2
        keep = [lax.dynamic_slice_in_dim(part, upper * half, half, 1) for part in found]
        give = [lax.dynamic_slice_in_dim(part, (1 - upper) * half, half, 1) for part in found]
        found = keep + [lax.ppermute(part, "dp", xor_pairs(count, bit)) for part in give]
    return found


def swap_tensor(values):
    return lax.ppermute(values, "tensor", [(0, 1), (1, 0)])


def sum_share(part):
    ranks = lax.axis_size("tensor")
    if ranks != 2:
        return lax.psum_scatter(part.astype(bf16), "tensor", scatter_dimension=1, tiled=True).astype(f32)
    share = part.shape[1] // 2
    me = lax.axis_index("tensor")
    mine = lax.dynamic_slice_in_dim(part, me * share, share, 1)
    theirs = lax.dynamic_slice_in_dim(part, (1 - me) * share, share, 1)
    return mine + swap_tensor(theirs.astype(bf16)).astype(f32)


def sum_whole(part):
    if lax.axis_size("tensor") != 2:
        return lax.psum(part.astype(bf16), "tensor").astype(f32)
    low = part.astype(bf16)
    return low.astype(f32) + swap_tensor(low).astype(f32)


def other_weight(weight):
    count, _ = dp_bits()
    half = weight.shape[0] // 2
    parity = lax.axis_index("dp") % 2
    got = swap_tensor(lax.dynamic_slice_in_dim(weight, parity * half, half, 0))
    also = lax.ppermute(got, "dp", xor_pairs(count, 1))
    even = parity == 0
    return jnp.where(even, got, also), jnp.where(even, also, got)


def ctx_scatter(block):
    return lax.psum_scatter(block, "ctx", scatter_dimension=0, tiled=True)


def gains_own(parts):
    if lax.axis_size("tensor") == 2:
        parts = parts + swap_tensor(parts)
    else:
        parts = lax.psum(parts, "tensor")
    count, bits = dp_bits()
    me = lax.axis_index("dp")
    for bit in bits:
        half = parts.shape[1] // 2
        upper = (me // bit) % 2
        keep = lax.dynamic_slice_in_dim(parts, upper * half, half, 1)
        give = lax.dynamic_slice_in_dim(parts, (1 - upper) * half, half, 1)
        parts = keep + lax.ppermute(give, "dp", xor_pairs(count, bit))
    return parts


def shards(
    block_in,
    attn_gain,
    query_weight,
    key_weight,
    value_weight,
    output_weight,
    mlp_gain,
    gate_weight,
    up_weight,
    down_weight,
    cotangent,
):
    seq_count, ctx_tok, width = block_in.shape
    ctx_ranks = lax.axis_size("ctx")
    tensor_ranks = lax.axis_size("tensor")
    share_len = ctx_tok // tensor_ranks
    share_start = lax.axis_index("tensor") * share_len
    rows = seq_count * ctx_tok
    query_cols = query_weight.shape[1]
    kv_cols = key_weight.shape[1]
    units = gate_weight.shape[1]
    ctx_at = lax.axis_index("ctx")
    deep = (seq_count, ctx_tok, width)

    def share_of(values):
        return lax.dynamic_slice_in_dim(values, share_start, share_len, 1)

    gain_first = attn_gain.astype(f32)
    gain_second = mlp_gain.astype(f32)
    flat_in = block_in.reshape(rows, width)
    cot_rows = cotangent.reshape(rows, width)
    positions = ctx_at * ctx_tok + jnp.arange(ctx_tok, dtype=jnp.int32)
    cosine, sine = rope_columns(positions)
    ones = jnp.ones((ctx_tok, kv_cols), f32)
    table = lambda one, rest: jnp.concatenate(
        [jnp.tile(one[:, :HD], (1, kv_cols // HD)), rest], axis=1
    )
    kv_cosine, kv_sine = table(cosine, ones), table(sine, ones * 0.0)

    normed, kv_own = norm_kv(
        flat_in, attn_gain[None], key_weight, value_weight, kv_cosine, kv_sine
    )
    kv_blocks = [kv_own]
    for back in range(1, ctx_ranks):
        kv_blocks.append(
            lax.ppermute(kv_own, "ctx", [(i, i + back) for i in range(ctx_ranks - back)])
        )
    queries = project_queries(normed, query_weight, cosine, sine)
    attended = attend(queries, kv_blocks, ctx_tok)
    branch = dot_nn(attended, output_weight)
    if tensor_ranks == 2:
        theirs = swap_tensor(attended)
        half = query_cols // 2
        low, high = other_weight(output_weight)
        branch = branch + dot_nn(theirs[:, :half], low) + dot_nn(theirs[:, half:], high)
    else:
        branch = lax.psum(branch, "tensor")
    hidden = flat_in.astype(f32) + branch
    r_second = lax.rsqrt(jnp.mean(hidden * hidden, axis=-1, keepdims=True) + norm_eps)
    normed_mlp = (hidden * r_second * gain_second).astype(bf16)

    unit = units // 4
    weights = (gate_weight, up_weight, down_weight)
    act_0, grads_0, *sums = mlp(normed_mlp, cot_rows, *weights, 0, unit, None, (1, 2))
    pack_1, *sums = mlp(normed_mlp, cot_rows, *weights, unit, unit, sums, (3,))
    pack_2, *sums = mlp(normed_mlp, cot_rows, *weights, 2 * unit, 2 * unit, sums, (3,))
    mlp_part, back_part = sums

    cot_cols = dp_columns(cot_rows)
    normed_cols = dp_columns(normed)
    attended_all = dp_rows(attended[None])
    nm_cols = dp_columns(normed_mlp)
    both = [cot_cols, nm_cols]
    first_sum = ctx_scatter(weight_grad(None, unit, 0, [cot_cols], (0,), dp_rows(act_0)))
    second_sum = ctx_scatter(weight_grad(None, 2 * unit, 0, [nm_cols], (0, 0), dp_rows(grads_0)))
    third_sum = ctx_scatter(weight_grad(None, 3 * unit, 0, both, (0, 1, 1), dp_rows(pack_1)))
    qkv_cols = query_cols + 2 * kv_cols
    attn_at = 6 * unit
    total = attn_at + qkv_cols + query_cols + 128
    last = weight_grad(None, total, 0, both, (0, 1, 1), dp_rows(pack_2))

    hidden_deep = hidden.reshape(deep)
    block_out = (share_of(hidden_deep) + sum_share(mlp_part.reshape(deep))).astype(bf16)
    unit_second = hidden * r_second
    mlp_gain_part = jnp.sum(back_part * unit_second, axis=0)
    scaled = gain_second * sum_whole(back_part)
    grad_hidden = cot_rows.astype(f32) + r_second * (
        scaled - unit_second * jnp.mean(scaled * unit_second, axis=-1, keepdims=True)
    )
    grad_branch = grad_hidden.astype(bf16)
    grad_attended = dot_nt(grad_branch, output_weight).astype(bf16)
    branch_cols = dp_columns(grad_branch)
    last = weight_grad(last, total, attn_at + qkv_cols, [branch_cols], (0,), attended_all)

    grad_query_raw, kv_sum, *kv_given = attend_back(
        queries, kv_blocks, grad_attended, cosine, sine, ctx_tok
    )
    for back, piece in enumerate(kv_given, 1):
        kv_sum = kv_sum + lax.ppermute(
            piece, "ctx", [(i + back, i) for i in range(ctx_ranks - back)]
        ).astype(f32)
    kv_sum = kv_sum.reshape(seq_count, ctx_tok, 2, kv_cols // HD, 2, HD // 2)
    first_half, second_half = kv_sum[..., 0, :], kv_sum[..., 1, :]
    cos_half = jnp.stack([cosine[:, : HD // 2], ones[:, : HD // 2]], axis=1)[:, :, None]
    sin_half = jnp.stack([sine[:, HD // 2 : HD], ones[:, : HD // 2] * 0.0], axis=1)[:, :, None]
    grad_kv_raw = (
        jnp.stack(
            [
                first_half * cos_half + second_half * sin_half,
                second_half * cos_half - first_half * sin_half,
            ],
            axis=-2,
        )
        .astype(bf16)
        .reshape(rows, 2 * kv_cols)
    )
    grad_raw = jnp.concatenate([grad_query_raw, grad_kv_raw], axis=1)
    last = weight_grad(last, total, attn_at, [normed_cols], (0,), dp_rows(grad_raw[None]))
    grad_normed_first = (
        dot_nt(grad_query_raw, query_weight)
        + dot_nt(grad_kv_raw[:, :kv_cols], key_weight)
        + dot_nt(grad_kv_raw[:, kv_cols:], value_weight)
    )
    full_in = flat_in.astype(f32)
    r_first = lax.rsqrt(jnp.mean(full_in * full_in, axis=-1, keepdims=True) + norm_eps)
    unit_first = full_in * r_first
    attn_gain_part = jnp.sum(grad_normed_first * unit_first, axis=0)
    gains = gains_own(jnp.stack([attn_gain_part, mlp_gain_part]))
    gain_block = jnp.pad(gains.T.astype(bf16), ((0, 0), (0, 126)))
    last = lax.dynamic_update_slice(last, gain_block, (0, total - 128))
    last_sum = ctx_scatter(last)

    scaled_first = gain_first * sum_share(grad_normed_first.reshape(deep))
    unit_share = share_of(unit_first.reshape(deep))
    input_grad = share_of(grad_hidden.reshape(deep)) + share_of(r_first.reshape(seq_count, ctx_tok, 1)) * (
        scaled_first - unit_share * jnp.mean(scaled_first * unit_share, axis=-1, keepdims=True)
    )

    def joined(*parts):
        return jnp.concatenate(parts, axis=1).astype(f32)

    grad_down = joined(first_sum, third_sum[:, :unit], last_sum[:, : 2 * unit]).T
    grad_gate = joined(
        second_sum[:, :unit], third_sum[:, unit : 2 * unit], last_sum[:, 2 * unit : 4 * unit]
    )
    grad_up = joined(second_sum[:, unit:], third_sum[:, 2 * unit :], last_sum[:, 4 * unit : attn_at])
    query_end = attn_at + query_cols
    key_end = query_end + kv_cols
    value_end = key_end + kv_cols
    cut = lambda first, end: last_sum[:, first:end].astype(f32)
    gains_out = cut(total - 128, total - 126)
    return (
        block_out,
        input_grad,
        gains_out[:, 0],
        cut(attn_at, query_end),
        cut(query_end, key_end),
        cut(key_end, value_end),
        cut(value_end, total - 128).T,
        gains_out[:, 1],
        grad_gate,
        grad_up,
        grad_down,
    )


def solution(mesh):
    in_specs = (
        P("dp", "ctx", None),
        P(),
        P(None, "tensor"),
        P(None, "tensor"),
        P(None, "tensor"),
        P("tensor", None),
        P(),
        P(None, "tensor"),
        P(None, "tensor"),
        P("tensor", None),
        P("dp", "ctx", None),
    )
    out_specs = (
        P("dp", ("ctx", "tensor"), None),
        P("dp", ("ctx", "tensor"), None),
        P(("dp", "ctx")),
        P(("dp", "ctx"), "tensor"),
        P(("dp", "ctx"), "tensor"),
        P(("dp", "ctx"), "tensor"),
        P("tensor", ("dp", "ctx")),
        P(("dp", "ctx")),
        P(("dp", "ctx"), "tensor"),
        P(("dp", "ctx"), "tensor"),
        P("tensor", ("dp", "ctx")),
    )
    return jax.shard_map(shards, mesh=mesh, in_specs=in_specs, out_specs=out_specs, check_vma=False)
```

```python
import jax
import jax.numpy as jnp
from jax import lax
from jax.experimental import pallas as pl
from jax.experimental.pallas import tpu as pltpu
from jax.sharding import PartitionSpec as P


HD = 64

norm_eps = 1e-05
rope_base = 500000.0
f32 = jnp.float32
bf16 = jnp.bfloat16


def rms_apply(values, gain):
    return values * lax.rsqrt(jnp.mean(values * values, axis=-1, keepdims=True) + norm_eps) * gain


def rope_tables(positions, head_size):
    half_width = head_size // 2
    frequency = rope_base ** (-jnp.arange(half_width, dtype=f32) * 2.0 / head_size)
    angles = positions.astype(f32)[:, None] * frequency[None, :]
    return (jnp.cos(angles)[:, None, :], jnp.sin(angles)[:, None, :])


def dot_nn(left, right):
    return lax.dot_general(left, right, (((1,), (0,)), ((), ())), preferred_element_type=f32)


def dot_tn(left, right):
    return lax.dot_general(left, right, (((0,), (0,)), ((), ())), preferred_element_type=f32)


def dot_nt(left, right):
    return lax.dot_general(left, right, (((1,), (1,)), ((), ())), preferred_element_type=f32)


def call(body, grid, in_specs, out_specs, out_shape, flops, moved, **rest):
    return pl.pallas_call(
        body,
        grid=grid,
        in_specs=in_specs,
        out_specs=out_specs,
        out_shape=out_shape,
        cost_estimate=pl.CostEstimate(flops=flops, bytes_accessed=moved, transcendentals=0),
        compiler_params=pltpu.CompilerParams(vmem_limit_bytes=56 << 20),
        **rest,
    )


def whole(shape):
    zeros = (0,) * len(shape)
    return pl.BlockSpec(shape, lambda *_: zeros, pipeline_mode=pl.Buffered(1))


def shape_of(shape, kind):
    return jax.ShapeDtypeStruct(shape, kind)


def turned(values, cosine, sine):
    at = lax.broadcasted_iota(jnp.int32, values.shape, 1) % HD
    swapped = jnp.where(
        at < HD // 2, pltpu.roll(values, 128 - HD // 2, 1), pltpu.roll(values, HD // 2, 1)
    )
    return values * cosine + swapped * sine


def rope_columns(positions):
    cosine, sine = rope_tables(positions, HD)
    cosine, sine = cosine[:, 0], sine[:, 0]
    return jnp.tile(cosine, (1, 4)), jnp.tile(jnp.concatenate([-sine, sine], axis=-1), (1, 2))


def norm_kv(rows, gain, key_weight, value_weight, cosine, sine):
    count, width = rows.shape
    cols = key_weight.shape[1]
    tokens = cosine.shape[0]

    def body(rows_ref, gain_ref, key_ref, value_ref, cos_ref, sin_ref, normed_ref, kv_ref):
        values = rows_ref[...].astype(f32)
        normed = rms_apply(values, gain_ref[...].astype(f32)).astype(bf16)
        normed_ref[...] = normed
        raw = jnp.concatenate([dot_nn(normed, key_ref[...]), dot_nn(normed, value_ref[...])], axis=1)
        for first in range(0, count, tokens):
            for at in range(0, 2 * cols, 128):
                part = raw[first : first + tokens, at : at + 128]
                kv_ref[first : first + tokens, at : at + 128] = turned(
                    part, cos_ref[:, at : at + 128], sin_ref[:, at : at + 128]
                ).astype(bf16)

    shapes = [rows.shape, gain.shape, key_weight.shape, value_weight.shape, cosine.shape, sine.shape]
    return call(
        body,
        (1,),
        [whole(s) for s in shapes],
        [whole(rows.shape), whole((count, 2 * cols))],
        [shape_of(rows.shape, bf16), shape_of((count, 2 * cols), bf16)],
        4 * count * width * cols,
        2 * (2 * count * width + 2 * width * cols),
    )(rows, gain, key_weight, value_weight, cosine, sine)


def tile_of(*sizes):
    for tile in (512, 256, 128):
        if all(size % tile == 0 for size in sizes):
            return tile
    raise ValueError("no tile")


def project_queries(normed, weight, cosine, sine):
    count, width = normed.shape
    cols = weight.shape[1]
    tokens = cosine.shape[0]
    tile = tile_of(cols)

    def body(normed_ref, weight_ref, cos_ref, sin_ref, out_ref):
        raw = dot_nn(normed_ref[...], weight_ref[...])
        for first in range(0, count, tokens):
            for at in range(0, tile, 128):
                out_ref[first : first + tokens, at : at + 128] = turned(
                    raw[first : first + tokens, at : at + 128], cos_ref[...], sin_ref[...]
                ).astype(bf16)

    return call(
        body,
        (cols // tile,),
        [
            whole(normed.shape),
            pl.BlockSpec((width, tile), lambda i: (0, i)),
            whole(cosine.shape),
            whole(sine.shape),
        ],
        pl.BlockSpec((count, tile), lambda i: (0, i)),
        shape_of((count, cols), bf16),
        2 * count * width * cols,
        2 * (count * width + width * cols),
    )(normed, weight, cosine, sine)


def scores_of(stacked, keys, ctx_at, scale):
    tokens = keys[0].shape[0]
    found = []
    for back, block in enumerate(keys):
        raw = dot_nt(stacked, block) * scale
        if back == 0:
            query_at = lax.broadcasted_iota(jnp.int32, raw.shape, 0) % tokens
            seen = query_at >= lax.broadcasted_iota(jnp.int32, raw.shape, 1)
            found.append(jnp.where(seen, raw, -1e30))
        else:
            found.append(raw + jnp.where(ctx_at >= back, 0.0, -1e30).astype(f32))
    most = jnp.max(found[0], axis=-1, keepdims=True)
    for masked in found[1:]:
        most = jnp.maximum(most, jnp.max(masked, axis=-1, keepdims=True))
    found = [jnp.exp(masked - most) for masked in found]
    total = sum(jnp.sum(part, axis=-1, keepdims=True) for part in found)
    inverse = 1.0 / total
    return [part * inverse for part in found]


def stack_heads(ref, head, group):
    first = head * group
    return jnp.concatenate(
        [ref[:, (first + g) * HD : (first + g + 1) * HD] for g in range(group)], axis=0
    )


def attend(queries, kv_blocks, tokens):
    count, cols = queries.shape
    kv_cols = kv_blocks[0].shape[1] // 2
    heads = kv_cols // HD
    group = cols // kv_cols
    scale = HD ** (-0.5)
    blocks = len(kv_blocks)

    def body(query_ref, *refs):
        out_ref = refs[-1]
        ctx_at = lax.axis_index("ctx")
        for head in range(heads):
            stacked = stack_heads(query_ref, head, group)
            at = head * HD
            keys = [ref[:, at : at + HD] for ref in refs[:blocks]]
            probs = scores_of(stacked, keys, ctx_at, scale)
            total = sum(
                dot_nn(part.astype(bf16), ref[:, kv_cols + at : kv_cols + at + HD])
                for part, ref in zip(probs, refs)
            )
            for g in range(group):
                first = (head * group + g) * HD
                out_ref[:, first : first + HD] = total[g * tokens : (g + 1) * tokens].astype(bf16)

    rows = lambda width: pl.BlockSpec((tokens, width), lambda i: (i, 0))
    return call(
        body,
        (count // tokens,),
        [rows(cols)] + [rows(2 * kv_cols)] * blocks,
        rows(cols),
        shape_of((count, cols), bf16),
        40 * count * cols * tokens * blocks,
        2 * count * (2 * cols + 2 * kv_cols * blocks),
    )(queries, *kv_blocks)


def attend_back(queries, kv_blocks, grad_attended, cosine, sine, tokens):
    count, cols = queries.shape
    kv_cols = kv_blocks[0].shape[1] // 2
    heads = kv_cols // HD
    group = cols // kv_cols
    scale = HD ** (-0.5)
    blocks = len(kv_blocks)

    def body(query_ref, grad_ref, cos_ref, sin_ref, *refs):
        kv_refs, query_out, kv_out = refs[:blocks], refs[blocks], refs[blocks + 1 : -1]
        turned_ref = refs[-1]
        ctx_at = lax.axis_index("ctx")
        for head in range(heads):
            stacked = stack_heads(query_ref, head, group)
            grads = stack_heads(grad_ref, head, group)
            at = head * HD
            keys = [ref[:, at : at + HD] for ref in kv_refs]
            values = [ref[:, kv_cols + at : kv_cols + at + HD] for ref in kv_refs]
            probs = scores_of(stacked, keys, ctx_at, scale)
            grad_probs = [dot_nt(grads, block) for block in values]
            inner = sum(
                jnp.sum(part * grad, axis=-1, keepdims=True)
                for part, grad in zip(probs, grad_probs)
            )
            total = 0.0
            for back in range(blocks):
                grad_scores = (probs[back] * (grad_probs[back] - inner)).astype(bf16)
                total = total + dot_nn(grad_scores, keys[back])
                kind = kv_out[back].dtype
                kv_out[back][:, at : at + HD] = (dot_tn(grad_scores, stacked) * scale).astype(kind)
                kv_out[back][:, kv_cols + at : kv_cols + at + HD] = dot_tn(
                    probs[back].astype(bf16), grads
                ).astype(kind)
            for g in range(group):
                first = (head * group + g) * HD
                turned_ref[:, first : first + HD] = total[g * tokens : (g + 1) * tokens] * scale
        for at in range(0, cols, 128):
            query_out[:, at : at + 128] = turned(
                turned_ref[:, at : at + 128], cos_ref[...], -sin_ref[...]
            ).astype(bf16)

    rows = lambda width: pl.BlockSpec((tokens, width), lambda i: (i, 0))
    return call(
        body,
        (count // tokens,),
        [rows(cols), rows(cols), whole(cosine.shape), whole(sine.shape)]
        + [rows(2 * kv_cols)] * blocks,
        [rows(cols)] + [rows(2 * kv_cols)] * blocks,
        [shape_of((count, cols), bf16)]
        + [shape_of((count, 2 * kv_cols), f32 if back == 0 else bf16) for back in range(blocks)],
        100 * count * cols * tokens * blocks,
        2 * count * (3 * cols + 4 * kv_cols * blocks),
        scratch_shapes=[pltpu.VMEM((tokens, cols), f32)],
    )(queries, grad_attended, cosine, sine, *kv_blocks)


def mlp(normed, cot, gate_weight, up_weight, down_weight, start, size, parts):
    count, width = normed.shape
    tile = tile_of(start, size)
    base = start // tile

    def body(normed_ref, cot_ref, gate_ref, up_ref, down_ref, *refs):
        out_refs, down_sum, back_sum = refs[:-2], refs[-2], refs[-1]
        gate = dot_nn(normed_ref[...], gate_ref[...])
        up = dot_nn(normed_ref[...], up_ref[...])
        grad = dot_nt(cot_ref[...], down_ref[...])
        sig = 1.0 / (1.0 + jnp.exp(-gate))
        silu = gate * sig
        activated = (silu * up).astype(bf16)
        grad_gate = (grad * up * sig * (1.0 + gate * (1.0 - sig))).astype(bf16)
        grad_up = (grad * silu).astype(bf16)
        made = [activated, grad_gate, grad_up]
        at = 0
        for ref in out_refs:
            for i in range(ref.shape[0]):
                ref[i] = made[at]
                at += 1
        first = pl.program_id(0) == 0

        @pl.when(first)
        def _():
            down_sum[...] = dot_nn(activated, down_ref[...])
            back_sum[...] = dot_nt(grad_gate, gate_ref[...]) + dot_nt(grad_up, up_ref[...])

        @pl.when(jnp.logical_not(first))
        def _():
            down_sum[...] += dot_nn(activated, down_ref[...])
            back_sum[...] += dot_nt(grad_gate, gate_ref[...]) + dot_nt(grad_up, up_ref[...])

    held = whole((count, width))
    columns = pl.BlockSpec((width, tile), lambda i: (0, base + i))
    return call(
        body,
        (size // tile,),
        [held, held, columns, columns, pl.BlockSpec((tile, width), lambda i: (base + i, 0))],
        [pl.BlockSpec((n, count, tile), lambda i: (0, 0, i)) for n in parts] + [held, held],
        [shape_of((n, count, size), bf16) for n in parts]
        + [shape_of((count, width), f32)] * 2,
        12 * count * width * size,
        2 * (3 * width * size + 3 * count * size + 6 * count * width),
    )(normed, cot, gate_weight, up_weight, down_weight)


def weight_grad(buffer, total, start, lefts, chosen, rights):
    entries, count, size = rights[0].shape
    own = lefts[0][0].shape[1]
    tile = tile_of(start, size)
    base, steps = start // tile, size // tile
    sources = len(rights)
    given = 0 if buffer is None else 1

    def body(*refs):
        out_ref = refs[-1]
        rights_at = refs[given + sources * len(lefts) : -1]

        def product(which):
            left = refs[given + sources * which : given + sources * (which + 1)]
            out_ref[...] = sum(dot_tn(a[...], b[0]) for a, b in zip(left, rights_at)).astype(bf16)

        for which in range(len(lefts)):
            if len(lefts) == 1:
                product(0)
            else:
                mine = [v for v in range(entries) if chosen[v] == which]
                v = pl.program_id(0)
                pl.when((v >= mine[0]) & (v <= mine[-1]))(lambda which=which: product(which))

    return call(
        body,
        (entries, steps),
        [pl.BlockSpec(memory_space=pl.ANY)] * given
        + [whole((count, own))] * (sources * len(lefts))
        + [pl.BlockSpec((1, count, tile), lambda v, i: (v, 0, i))] * sources,
        pl.BlockSpec((own, tile), lambda v, i: (0, base + v * steps + i)),
        shape_of((own, total), bf16),
        2 * entries * sources * count * own * size,
        2 * entries * size * (sources * count + own),
        input_output_aliases={0: 0} if given else {},
    )(*([] if buffer is None else [buffer]), *(p for left in lefts for p in left), *rights)


def xor_pairs(count, bit):
    return [(i, i ^ bit) for i in range(count)]


def dp_bits():
    count = lax.axis_size("dp")
    bits = []
    bit = count // 2
    while bit:
        bits.append(bit)
        bit //= 2
    return count, bits


def moved_dp(parts, bit):
    found = []
    for part in parts:
        found.append(lax.ppermute(part, "dp", xor_pairs(lax.axis_size("dp"), bit)))
    return found


def dp_rows(rows):
    _, bits = dp_bits()
    found = [rows]
    for bit in bits:
        found = found + moved_dp(found, bit)
    return found


def dp_columns(rows):
    _, bits = dp_bits()
    me = lax.axis_index("dp")
    found = [rows]
    for bit in bits:
        half = found[0].shape[1] // 2
        upper = (me // bit) % 2
        keep = [lax.dynamic_slice_in_dim(part, upper * half, half, 1) for part in found]
        give = [lax.dynamic_slice_in_dim(part, (1 - upper) * half, half, 1) for part in found]
        found = keep + moved_dp(give, bit)
    return found


def swap_tensor(values):
    return lax.ppermute(values, "tensor", [(0, 1), (1, 0)])


def sum_share(part):
    ranks = lax.axis_size("tensor")
    if ranks != 2:
        return lax.psum_scatter(part.astype(bf16), "tensor", scatter_dimension=1, tiled=True).astype(f32)
    share = part.shape[1] // 2
    me = lax.axis_index("tensor")
    mine = lax.dynamic_slice_in_dim(part, me * share, share, 1)
    theirs = lax.dynamic_slice_in_dim(part, (1 - me) * share, share, 1)
    return mine + swap_tensor(theirs.astype(bf16)).astype(f32)


def sum_whole(part):
    if lax.axis_size("tensor") != 2:
        return lax.psum(part.astype(bf16), "tensor").astype(f32)
    low = part.astype(bf16)
    return low.astype(f32) + swap_tensor(low).astype(f32)


def other_weight(weight):
    _, _ = dp_bits()
    half = weight.shape[0] // 2
    parity = lax.axis_index("dp") % 2
    got = swap_tensor(lax.dynamic_slice_in_dim(weight, parity * half, half, 0))
    also = moved_dp([got], 1)[0]
    even = parity == 0
    return jnp.where(even, got, also), jnp.where(even, also, got)


def ctx_scatter(block):
    return lax.psum_scatter(block, "ctx", scatter_dimension=0, tiled=True)


def gains_own(parts):
    if lax.axis_size("tensor") == 2:
        parts = parts + swap_tensor(parts)
    else:
        parts = lax.psum(parts, "tensor")
    count, bits = dp_bits()
    me = lax.axis_index("dp")
    for bit in bits:
        half = parts.shape[1] // 2
        upper = (me // bit) % 2
        keep = lax.dynamic_slice_in_dim(parts, upper * half, half, 1)
        give = lax.dynamic_slice_in_dim(parts, (1 - upper) * half, half, 1)
        parts = keep + lax.ppermute(give, "dp", xor_pairs(count, bit))
    return parts


def shards(
    block_in,
    attn_gain,
    query_weight,
    key_weight,
    value_weight,
    output_weight,
    mlp_gain,
    gate_weight,
    up_weight,
    down_weight,
    cotangent,
):
    seq_count, ctx_tok, width = block_in.shape
    ctx_ranks = lax.axis_size("ctx")
    tensor_ranks = lax.axis_size("tensor")
    share_len = ctx_tok // tensor_ranks
    share_start = lax.axis_index("tensor") * share_len
    rows = seq_count * ctx_tok
    query_cols = query_weight.shape[1]
    kv_cols = key_weight.shape[1]
    units = gate_weight.shape[1]
    ctx_at = lax.axis_index("ctx")
    deep = (seq_count, ctx_tok, width)

    def share_of(values):
        return lax.dynamic_slice_in_dim(values, share_start, share_len, 1)

    gain_first = attn_gain.astype(f32)
    gain_second = mlp_gain.astype(f32)
    flat_in = block_in.reshape(rows, width)
    cot_rows = cotangent.reshape(rows, width)
    positions = ctx_at * ctx_tok + jnp.arange(ctx_tok, dtype=jnp.int32)
    cosine, sine = rope_columns(positions)
    ones = jnp.ones((ctx_tok, kv_cols), f32)
    table = lambda one, rest: jnp.concatenate(
        [jnp.tile(one[:, :HD], (1, kv_cols // HD)), rest], axis=1
    )
    kv_cosine, kv_sine = table(cosine, ones), table(sine, ones * 0.0)

    normed, kv_own = norm_kv(flat_in, attn_gain[None], key_weight, value_weight, kv_cosine, kv_sine)
    kv_blocks = [kv_own]
    for back in range(1, ctx_ranks):
        kv_blocks.append(
            lax.ppermute(kv_own, "ctx", [(i, i + back) for i in range(ctx_ranks - back)])
        )
    queries = project_queries(normed, query_weight, cosine, sine)
    attended = attend(queries, kv_blocks, ctx_tok)
    branch = dot_nn(attended, output_weight)
    if tensor_ranks == 2:
        theirs = swap_tensor(attended)
        half = query_cols // 2
        low, high = other_weight(output_weight)
        branch = branch + dot_nn(theirs[:, :half], low) + dot_nn(theirs[:, half:], high)
    else:
        branch = lax.psum(branch, "tensor")
    hidden = flat_in.astype(f32) + branch
    r_second = lax.rsqrt(jnp.mean(hidden * hidden, axis=-1, keepdims=True) + norm_eps)
    normed_mlp = (hidden * r_second * gain_second).astype(bf16)

    unit = units // 4
    weights = (gate_weight, up_weight, down_weight)
    act_0, grads_0, down_0, back_0 = mlp(normed_mlp, cot_rows, *weights, 0, unit, (1, 2))
    pack_1, down_1, back_1 = mlp(normed_mlp, cot_rows, *weights, unit, unit, (3,))
    pack_2, down_2, back_2 = mlp(normed_mlp, cot_rows, *weights, 2 * unit, 2 * unit, (3,))
    mlp_part = down_0 + down_1 + down_2
    back_part = back_0 + back_1 + back_2

    cot_cols = dp_columns(cot_rows)
    normed_cols = dp_columns(normed)
    attended_all = dp_rows(attended[None])
    nm_cols = dp_columns(normed_mlp)
    both = [cot_cols, nm_cols]
    act_0, grads_0 = dp_rows(act_0), dp_rows(grads_0)
    pack_1, pack_2 = dp_rows(pack_1), dp_rows(pack_2)
    wg_0 = weight_grad(None, unit, 0, [cot_cols], (0,), act_0)
    wg_1 = weight_grad(None, 2 * unit, 0, [nm_cols], (0, 0), grads_0)
    wg_2 = weight_grad(None, 3 * unit, 0, both, (0, 1, 1), pack_1)
    wg_3 = weight_grad(None, 6 * unit, 0, both, (0, 1, 1), pack_2)
    first_sum = ctx_scatter(wg_0)
    second_sum = ctx_scatter(wg_1)
    third_sum = ctx_scatter(wg_2)
    fourth_sum = ctx_scatter(wg_3)
    qkv_cols = query_cols + 2 * kv_cols
    total = qkv_cols + query_cols + 128

    hidden_deep = hidden.reshape(deep)
    block_out = (share_of(hidden_deep) + sum_share(mlp_part.reshape(deep))).astype(bf16)
    unit_second = hidden * r_second
    mlp_gain_part = jnp.sum(back_part * unit_second, axis=0)
    scaled = gain_second * sum_whole(back_part)
    grad_hidden = cot_rows.astype(f32) + r_second * (
        scaled - unit_second * jnp.mean(scaled * unit_second, axis=-1, keepdims=True)
    )
    grad_branch = grad_hidden.astype(bf16)
    grad_attended = dot_nt(grad_branch, output_weight).astype(bf16)
    branch_cols = dp_columns(grad_branch)
    last = weight_grad(None, total, qkv_cols, [branch_cols], (0,), attended_all)

    grad_query_raw, kv_sum, *kv_given = attend_back(
        queries, kv_blocks, grad_attended, cosine, sine, ctx_tok
    )
    for back, piece in enumerate(kv_given, 1):
        given = lax.ppermute(piece, "ctx", [(i + back, i) for i in range(ctx_ranks - back)])
        kv_sum = kv_sum + given.astype(f32)
    kv_sum = kv_sum.reshape(seq_count, ctx_tok, 2, kv_cols // HD, 2, HD // 2)
    first_half, second_half = kv_sum[..., 0, :], kv_sum[..., 1, :]
    cos_half = jnp.stack([cosine[:, : HD // 2], ones[:, : HD // 2]], axis=1)[:, :, None]
    sin_half = jnp.stack([sine[:, HD // 2 : HD], ones[:, : HD // 2] * 0.0], axis=1)[:, :, None]
    grad_kv_raw = (
        jnp.stack(
            [
                first_half * cos_half + second_half * sin_half,
                second_half * cos_half - first_half * sin_half,
            ],
            axis=-2,
        )
        .astype(bf16)
        .reshape(rows, 2 * kv_cols)
    )
    grad_raw = jnp.concatenate([grad_query_raw, grad_kv_raw], axis=1)
    raw_all = dp_rows(grad_raw[None])
    last = weight_grad(last, total, 0, [normed_cols], (0,), raw_all)
    grad_normed_first = (
        dot_nt(grad_query_raw, query_weight)
        + dot_nt(grad_kv_raw[:, :kv_cols], key_weight)
        + dot_nt(grad_kv_raw[:, kv_cols:], value_weight)
    )
    full_in = flat_in.astype(f32)
    r_first = lax.rsqrt(jnp.mean(full_in * full_in, axis=-1, keepdims=True) + norm_eps)
    unit_first = full_in * r_first
    attn_gain_part = jnp.sum(grad_normed_first * unit_first, axis=0)
    gains = gains_own(jnp.stack([attn_gain_part, mlp_gain_part]))
    gain_block = jnp.pad(gains.T.astype(bf16), ((0, 0), (0, 126)))
    last = lax.dynamic_update_slice(last, gain_block, (0, total - 128))
    last_sum = ctx_scatter(last)

    scaled_first = gain_first * sum_share(grad_normed_first.reshape(deep))
    unit_share = share_of(unit_first.reshape(deep))
    input_grad = share_of(grad_hidden.reshape(deep)) + share_of(r_first.reshape(seq_count, ctx_tok, 1)) * (
        scaled_first - unit_share * jnp.mean(scaled_first * unit_share, axis=-1, keepdims=True)
    )

    def joined(*parts):
        return jnp.concatenate(parts, axis=1).astype(f32)

    grad_down = joined(first_sum, third_sum[:, :unit], fourth_sum[:, : 2 * unit]).T
    grad_gate = joined(
        second_sum[:, :unit], third_sum[:, unit : 2 * unit], fourth_sum[:, 2 * unit : 4 * unit]
    )
    grad_up = joined(second_sum[:, unit:], third_sum[:, 2 * unit :], fourth_sum[:, 4 * unit :])
    query_end = query_cols
    key_end = query_end + kv_cols
    value_end = key_end + kv_cols
    cut = lambda first, end: last_sum[:, first:end].astype(f32)
    gains_out = cut(total - 128, total - 126)
    return (
        block_out,
        input_grad,
        gains_out[:, 0],
        cut(0, query_end),
        cut(query_end, key_end),
        cut(key_end, value_end),
        cut(value_end, total - 128).T,
        gains_out[:, 1],
        grad_gate,
        grad_up,
        grad_down,
    )


def solution(mesh):
    in_specs = (
        P("dp", "ctx", None),
        P(),
        P(None, "tensor"),
        P(None, "tensor"),
        P(None, "tensor"),
        P("tensor", None),
        P(),
        P(None, "tensor"),
        P(None, "tensor"),
        P("tensor", None),
        P("dp", "ctx", None),
    )
    out_specs = (
        P("dp", ("ctx", "tensor"), None),
        P("dp", ("ctx", "tensor"), None),
        P(("dp", "ctx")),
        P(("dp", "ctx"), "tensor"),
        P(("dp", "ctx"), "tensor"),
        P(("dp", "ctx"), "tensor"),
        P("tensor", ("dp", "ctx")),
        P(("dp", "ctx")),
        P(("dp", "ctx"), "tensor"),
        P(("dp", "ctx"), "tensor"),
        P("tensor", ("dp", "ctx")),
    )

    return jax.shard_map(shards, mesh=mesh, in_specs=in_specs, out_specs=out_specs, check_vma=False)
```

```python
import jax
import jax.numpy as jnp
from jax import lax
from jax.experimental import pallas as pl
from jax.experimental.pallas import tpu as pltpu
from jax.sharding import PartitionSpec as P


HD = 64

norm_eps = 1e-05
rope_base = 500000.0
f32 = jnp.float32
bf16 = jnp.bfloat16


def rms_apply(values, gain):
    return values * lax.rsqrt(jnp.mean(values * values, axis=-1, keepdims=True) + norm_eps) * gain


def rope_tables(positions, head_size):
    half_width = head_size // 2
    frequency = rope_base ** (-jnp.arange(half_width, dtype=f32) * 2.0 / head_size)
    angles = positions.astype(f32)[:, None] * frequency[None, :]
    return (jnp.cos(angles)[:, None, :], jnp.sin(angles)[:, None, :])


def dot_nn(left, right):
    return lax.dot_general(left, right, (((1,), (0,)), ((), ())), preferred_element_type=f32)


def dot_tn(left, right):
    return lax.dot_general(left, right, (((0,), (0,)), ((), ())), preferred_element_type=f32)


def dot_nt(left, right):
    return lax.dot_general(left, right, (((1,), (1,)), ((), ())), preferred_element_type=f32)


def call(body, grid, in_specs, out_specs, out_shape, flops, moved, **rest):
    return pl.pallas_call(
        body,
        grid=grid,
        in_specs=in_specs,
        out_specs=out_specs,
        out_shape=out_shape,
        cost_estimate=pl.CostEstimate(flops=flops, bytes_accessed=moved, transcendentals=0),
        compiler_params=pltpu.CompilerParams(vmem_limit_bytes=56 << 20),
        **rest,
    )


def whole(shape):
    zeros = (0,) * len(shape)
    return pl.BlockSpec(shape, lambda *_: zeros, pipeline_mode=pl.Buffered(1))


def shape_of(shape, kind):
    return jax.ShapeDtypeStruct(shape, kind)


def turned(values, cosine, sine):
    at = lax.broadcasted_iota(jnp.int32, values.shape, 1) % HD
    swapped = jnp.where(
        at < HD // 2, pltpu.roll(values, 128 - HD // 2, 1), pltpu.roll(values, HD // 2, 1)
    )
    return values * cosine + swapped * sine


def rope_columns(positions):
    cosine, sine = rope_tables(positions, HD)
    cosine, sine = cosine[:, 0], sine[:, 0]
    return jnp.tile(cosine, (1, 4)), jnp.tile(jnp.concatenate([-sine, sine], axis=-1), (1, 2))


def norm_kv(rows, gain, key_weight, value_weight, cosine, sine):
    count, width = rows.shape
    cols = key_weight.shape[1]
    tokens = cosine.shape[0]

    def body(rows_ref, gain_ref, key_ref, value_ref, cos_ref, sin_ref, normed_ref, kv_ref):
        values = rows_ref[...].astype(f32)
        normed = rms_apply(values, gain_ref[...].astype(f32)).astype(bf16)
        normed_ref[...] = normed
        raw = jnp.concatenate([dot_nn(normed, key_ref[...]), dot_nn(normed, value_ref[...])], axis=1)
        for first in range(0, count, tokens):
            for at in range(0, 2 * cols, 128):
                part = raw[first : first + tokens, at : at + 128]
                kv_ref[first : first + tokens, at : at + 128] = turned(
                    part, cos_ref[:, at : at + 128], sin_ref[:, at : at + 128]
                ).astype(bf16)

    shapes = [rows.shape, gain.shape, key_weight.shape, value_weight.shape, cosine.shape, sine.shape]
    return call(
        body,
        (1,),
        [whole(s) for s in shapes],
        [whole(rows.shape), whole((count, 2 * cols))],
        [shape_of(rows.shape, bf16), shape_of((count, 2 * cols), bf16)],
        4 * count * width * cols,
        2 * (2 * count * width + 2 * width * cols),
    )(rows, gain, key_weight, value_weight, cosine, sine)


def tile_of(*sizes):
    for tile in (512, 256, 128):
        if all(size % tile == 0 for size in sizes):
            return tile
    raise ValueError("no tile")


def project_queries(normed, weight, cosine, sine):
    count, width = normed.shape
    cols = weight.shape[1]
    tokens = cosine.shape[0]
    tile = tile_of(cols)

    def body(normed_ref, weight_ref, cos_ref, sin_ref, out_ref):
        raw = dot_nn(normed_ref[...], weight_ref[...])
        for first in range(0, count, tokens):
            for at in range(0, tile, 128):
                out_ref[first : first + tokens, at : at + 128] = turned(
                    raw[first : first + tokens, at : at + 128], cos_ref[...], sin_ref[...]
                ).astype(bf16)

    return call(
        body,
        (cols // tile,),
        [
            whole(normed.shape),
            pl.BlockSpec((width, tile), lambda i: (0, i)),
            whole(cosine.shape),
            whole(sine.shape),
        ],
        pl.BlockSpec((count, tile), lambda i: (0, i)),
        shape_of((count, cols), bf16),
        2 * count * width * cols,
        2 * (count * width + width * cols),
    )(normed, weight, cosine, sine)


def scores_of(stacked, keys, ctx_at, scale):
    tokens = keys[0].shape[0]
    found = []
    for back, block in enumerate(keys):
        raw = dot_nt(stacked, block) * scale
        if back == 0:
            query_at = lax.broadcasted_iota(jnp.int32, raw.shape, 0) % tokens
            seen = query_at >= lax.broadcasted_iota(jnp.int32, raw.shape, 1)
            found.append(jnp.where(seen, raw, -1e30))
        else:
            found.append(raw + jnp.where(ctx_at >= back, 0.0, -1e30).astype(f32))
    most = jnp.max(found[0], axis=-1, keepdims=True)
    for masked in found[1:]:
        most = jnp.maximum(most, jnp.max(masked, axis=-1, keepdims=True))
    found = [jnp.exp(masked - most) for masked in found]
    total = sum(jnp.sum(part, axis=-1, keepdims=True) for part in found)
    inverse = 1.0 / total
    return [part * inverse for part in found]


def stack_heads(ref, head, group):
    first = head * group
    return jnp.concatenate(
        [ref[:, (first + g) * HD : (first + g + 1) * HD] for g in range(group)], axis=0
    )


def attend(queries, kv_blocks, tokens):
    count, cols = queries.shape
    kv_cols = kv_blocks[0].shape[1] // 2
    heads = kv_cols // HD
    group = cols // kv_cols
    scale = HD ** (-0.5)
    blocks = len(kv_blocks)

    def body(query_ref, *refs):
        out_ref = refs[-1]
        ctx_at = lax.axis_index("ctx")
        for head in range(heads):
            stacked = stack_heads(query_ref, head, group)
            at = head * HD
            keys = [ref[:, at : at + HD] for ref in refs[:blocks]]
            probs = scores_of(stacked, keys, ctx_at, scale)
            total = sum(
                dot_nn(part.astype(bf16), ref[:, kv_cols + at : kv_cols + at + HD])
                for part, ref in zip(probs, refs)
            )
            for g in range(group):
                first = (head * group + g) * HD
                out_ref[:, first : first + HD] = total[g * tokens : (g + 1) * tokens].astype(bf16)

    rows = lambda width: pl.BlockSpec((tokens, width), lambda i: (i, 0))
    return call(
        body,
        (count // tokens,),
        [rows(cols)] + [rows(2 * kv_cols)] * blocks,
        rows(cols),
        shape_of((count, cols), bf16),
        40 * count * cols * tokens * blocks,
        2 * count * (2 * cols + 2 * kv_cols * blocks),
    )(queries, *kv_blocks)


def attend_back(queries, kv_blocks, grad_attended, cosine, sine, tokens):
    count, cols = queries.shape
    kv_cols = kv_blocks[0].shape[1] // 2
    heads = kv_cols // HD
    group = cols // kv_cols
    scale = HD ** (-0.5)
    blocks = len(kv_blocks)

    def body(query_ref, grad_ref, cos_ref, sin_ref, *refs):
        kv_refs, query_out, kv_out = refs[:blocks], refs[blocks], refs[blocks + 1 : -1]
        turned_ref = refs[-1]
        ctx_at = lax.axis_index("ctx")
        for head in range(heads):
            stacked = stack_heads(query_ref, head, group)
            grads = stack_heads(grad_ref, head, group)
            at = head * HD
            keys = [ref[:, at : at + HD] for ref in kv_refs]
            values = [ref[:, kv_cols + at : kv_cols + at + HD] for ref in kv_refs]
            probs = scores_of(stacked, keys, ctx_at, scale)
            grad_probs = [dot_nt(grads, block) for block in values]
            inner = sum(
                jnp.sum(part * grad, axis=-1, keepdims=True)
                for part, grad in zip(probs, grad_probs)
            )
            total = 0.0
            for back in range(blocks):
                grad_scores = (probs[back] * (grad_probs[back] - inner)).astype(bf16)
                total = total + dot_nn(grad_scores, keys[back])
                kind = kv_out[back].dtype
                kv_out[back][:, at : at + HD] = (dot_tn(grad_scores, stacked) * scale).astype(kind)
                kv_out[back][:, kv_cols + at : kv_cols + at + HD] = dot_tn(
                    probs[back].astype(bf16), grads
                ).astype(kind)
            for g in range(group):
                first = (head * group + g) * HD
                turned_ref[:, first : first + HD] = total[g * tokens : (g + 1) * tokens] * scale
        for at in range(0, cols, 128):
            query_out[:, at : at + 128] = turned(
                turned_ref[:, at : at + 128], cos_ref[...], -sin_ref[...]
            ).astype(bf16)

    rows = lambda width: pl.BlockSpec((tokens, width), lambda i: (i, 0))
    return call(
        body,
        (count // tokens,),
        [rows(cols), rows(cols), whole(cosine.shape), whole(sine.shape)]
        + [rows(2 * kv_cols)] * blocks,
        [rows(cols)] + [rows(2 * kv_cols)] * blocks,
        [shape_of((count, cols), bf16)]
        + [shape_of((count, 2 * kv_cols), f32 if back == 0 else bf16) for back in range(blocks)],
        100 * count * cols * tokens * blocks,
        2 * count * (3 * cols + 4 * kv_cols * blocks),
        scratch_shapes=[pltpu.VMEM((tokens, cols), f32)],
    )(queries, grad_attended, cosine, sine, *kv_blocks)


def mlp(normed, cot, gate_weight, up_weight, down_weight, start, size, parts):
    count, width = normed.shape
    tile = tile_of(start, size)
    base = start // tile

    def body(normed_ref, cot_ref, gate_ref, up_ref, down_ref, *refs):
        out_refs, down_sum, back_sum = refs[:-2], refs[-2], refs[-1]
        gate = dot_nn(normed_ref[...], gate_ref[...])
        up = dot_nn(normed_ref[...], up_ref[...])
        grad = dot_nt(cot_ref[...], down_ref[...])
        sig = 1.0 / (1.0 + jnp.exp(-gate))
        silu = gate * sig
        activated = (silu * up).astype(bf16)
        grad_gate = (grad * up * sig * (1.0 + gate * (1.0 - sig))).astype(bf16)
        grad_up = (grad * silu).astype(bf16)
        made = [activated, grad_gate, grad_up]
        at = 0
        for ref in out_refs:
            for i in range(ref.shape[0]):
                ref[i] = made[at]
                at += 1
        first = pl.program_id(0) == 0

        @pl.when(first)
        def _():
            down_sum[...] = dot_nn(activated, down_ref[...])
            back_sum[...] = dot_nt(grad_gate, gate_ref[...]) + dot_nt(grad_up, up_ref[...])

        @pl.when(jnp.logical_not(first))
        def _():
            down_sum[...] += dot_nn(activated, down_ref[...])
            back_sum[...] += dot_nt(grad_gate, gate_ref[...]) + dot_nt(grad_up, up_ref[...])

    held = whole((count, width))
    columns = pl.BlockSpec((width, tile), lambda i: (0, base + i))
    return call(
        body,
        (size // tile,),
        [held, held, columns, columns, pl.BlockSpec((tile, width), lambda i: (base + i, 0))],
        [pl.BlockSpec((n, count, tile), lambda i: (0, 0, i)) for n in parts] + [held, held],
        [shape_of((n, count, size), bf16) for n in parts]
        + [shape_of((count, width), f32)] * 2,
        12 * count * width * size,
        2 * (3 * width * size + 3 * count * size + 6 * count * width),
    )(normed, cot, gate_weight, up_weight, down_weight)


def weight_grad(buffer, total, start, lefts, chosen, rights):
    entries, count, size = rights[0].shape
    own = lefts[0][0].shape[1]
    tile = tile_of(start, size)
    base, steps = start // tile, size // tile
    sources = len(rights)
    given = 0 if buffer is None else 1

    def body(*refs):
        out_ref = refs[-1]
        rights_at = refs[given + sources * len(lefts) : -1]

        def product(which):
            left = refs[given + sources * which : given + sources * (which + 1)]
            out_ref[...] = sum(dot_tn(a[...], b[0]) for a, b in zip(left, rights_at)).astype(bf16)

        for which in range(len(lefts)):
            if len(lefts) == 1:
                product(0)
            else:
                mine = [v for v in range(entries) if chosen[v] == which]
                v = pl.program_id(0)
                pl.when((v >= mine[0]) & (v <= mine[-1]))(lambda which=which: product(which))

    return call(
        body,
        (entries, steps),
        [pl.BlockSpec(memory_space=pl.ANY)] * given
        + [whole((count, own))] * (sources * len(lefts))
        + [pl.BlockSpec((1, count, tile), lambda v, i: (v, 0, i))] * sources,
        pl.BlockSpec((own, tile), lambda v, i: (0, base + v * steps + i)),
        shape_of((own, total), bf16),
        2 * entries * sources * count * own * size,
        2 * entries * size * (sources * count + own),
        input_output_aliases={0: 0} if given else {},
    )(*([] if buffer is None else [buffer]), *(p for left in lefts for p in left), *rights)


def xor_pairs(count, bit):
    return [(i, i ^ bit) for i in range(count)]


def dp_bits():
    count = lax.axis_size("dp")
    bits = []
    bit = count // 2
    while bit:
        bits.append(bit)
        bit //= 2
    return count, bits


def moved_dp(parts, bit):
    found = []
    for part in parts:
        found.append(lax.ppermute(part, "dp", xor_pairs(lax.axis_size("dp"), bit)))
    return found


def dp_rows(rows):
    _, bits = dp_bits()
    found = [rows]
    for bit in bits:
        found = found + moved_dp(found, bit)
    return found


def dp_columns(rows):
    _, bits = dp_bits()
    me = lax.axis_index("dp")
    found = [rows]
    for bit in bits:
        half = found[0].shape[1] // 2
        upper = (me // bit) % 2
        keep = [lax.dynamic_slice_in_dim(part, upper * half, half, 1) for part in found]
        give = [lax.dynamic_slice_in_dim(part, (1 - upper) * half, half, 1) for part in found]
        found = keep + moved_dp(give, bit)
    return found


def swap_tensor(values):
    return lax.ppermute(values, "tensor", [(0, 1), (1, 0)])


def sum_share(part):
    ranks = lax.axis_size("tensor")
    if ranks != 2:
        return lax.psum_scatter(part.astype(bf16), "tensor", scatter_dimension=1, tiled=True).astype(f32)
    share = part.shape[1] // 2
    me = lax.axis_index("tensor")
    mine = lax.dynamic_slice_in_dim(part, me * share, share, 1)
    theirs = lax.dynamic_slice_in_dim(part, (1 - me) * share, share, 1)
    return mine + swap_tensor(theirs.astype(bf16)).astype(f32)


def sum_whole(part):
    if lax.axis_size("tensor") != 2:
        return lax.psum(part.astype(bf16), "tensor").astype(f32)
    low = part.astype(bf16)
    return low.astype(f32) + swap_tensor(low).astype(f32)


def other_weight(weight):
    count, _ = dp_bits()
    size = weight.shape[0] // count
    own = lax.dynamic_slice_in_dim(weight, lax.axis_index("dp") * size, size, 0)
    return dp_rows(swap_tensor(own))


def join_branch(base, theirs, pieces, gain):
    count, width = base.shape
    size = pieces[0].shape[0]
    order = [0]
    for bit in dp_bits()[1]:
        order = order + [at ^ bit for at in order]

    def body(base_ref, theirs_ref, gain_ref, *refs):
        piece_refs, (hidden_ref, scale_ref, normed_ref) = refs[:-3], refs[-3:]
        me = lax.axis_index("dp")
        total = base_ref[...]
        for flip, ref in zip(order, piece_refs):
            at = pl.multiple_of((me ^ flip) * size, size)
            total = total + dot_nn(theirs_ref[:, pl.ds(at, size)], ref[...])
        hidden_ref[...] = total
        scale = lax.rsqrt(jnp.mean(total * total, axis=-1, keepdims=True) + norm_eps)
        scale_ref[...] = scale
        normed_ref[...] = (total * scale * gain_ref[...].astype(f32)).astype(bf16)

    return call(
        body,
        (1,),
        [whole(base.shape), whole(theirs.shape), whole(gain.shape)] + [whole(p.shape) for p in pieces],
        [whole(base.shape), whole((count, 1)), whole(base.shape)],
        [shape_of(base.shape, f32), shape_of((count, 1), f32), shape_of(base.shape, bf16)],
        2 * count * width * size * len(pieces),
        2 * (5 * count * width + width * size * len(pieces)),
    )(base, theirs, gain, *pieces)


def ctx_scatter(block):
    return lax.psum_scatter(block, "ctx", scatter_dimension=0, tiled=True)


def gains_own(parts):
    if lax.axis_size("tensor") == 2:
        parts = parts + swap_tensor(parts)
    else:
        parts = lax.psum(parts, "tensor")
    count, bits = dp_bits()
    me = lax.axis_index("dp")
    for bit in bits:
        half = parts.shape[1] // 2
        upper = (me // bit) % 2
        keep = lax.dynamic_slice_in_dim(parts, upper * half, half, 1)
        give = lax.dynamic_slice_in_dim(parts, (1 - upper) * half, half, 1)
        parts = keep + lax.ppermute(give, "dp", xor_pairs(count, bit))
    return parts


def shards(
    block_in,
    attn_gain,
    query_weight,
    key_weight,
    value_weight,
    output_weight,
    mlp_gain,
    gate_weight,
    up_weight,
    down_weight,
    cotangent,
):
    seq_count, ctx_tok, width = block_in.shape
    ctx_ranks = lax.axis_size("ctx")
    tensor_ranks = lax.axis_size("tensor")
    share_len = ctx_tok // tensor_ranks
    share_start = lax.axis_index("tensor") * share_len
    rows = seq_count * ctx_tok
    query_cols = query_weight.shape[1]
    kv_cols = key_weight.shape[1]
    units = gate_weight.shape[1]
    ctx_at = lax.axis_index("ctx")
    deep = (seq_count, ctx_tok, width)

    def share_of(values):
        return lax.dynamic_slice_in_dim(values, share_start, share_len, 1)

    gain_first = attn_gain.astype(f32)
    gain_second = mlp_gain.astype(f32)
    flat_in = block_in.reshape(rows, width)
    cot_rows = cotangent.reshape(rows, width)
    positions = ctx_at * ctx_tok + jnp.arange(ctx_tok, dtype=jnp.int32)
    cosine, sine = rope_columns(positions)
    ones = jnp.ones((ctx_tok, kv_cols), f32)
    table = lambda one, rest: jnp.concatenate(
        [jnp.tile(one[:, :HD], (1, kv_cols // HD)), rest], axis=1
    )
    kv_cosine, kv_sine = table(cosine, ones), table(sine, ones * 0.0)

    normed, kv_own = norm_kv(flat_in, attn_gain[None], key_weight, value_weight, kv_cosine, kv_sine)
    kv_blocks = [kv_own]
    for back in range(1, ctx_ranks):
        kv_blocks.append(
            lax.ppermute(kv_own, "ctx", [(i, i + back) for i in range(ctx_ranks - back)])
        )
    queries = project_queries(normed, query_weight, cosine, sine)
    attended = attend(queries, kv_blocks, ctx_tok)
    branch = dot_nn(attended, output_weight)
    if tensor_ranks == 2:
        theirs = swap_tensor(attended)
        pieces = other_weight(output_weight)
        hidden, r_second, normed_mlp = join_branch(
            flat_in.astype(f32) + branch, theirs, pieces, mlp_gain[None]
        )
    else:
        hidden = flat_in.astype(f32) + lax.psum(branch, "tensor")
        r_second = lax.rsqrt(jnp.mean(hidden * hidden, axis=-1, keepdims=True) + norm_eps)
        normed_mlp = (hidden * r_second * gain_second).astype(bf16)

    unit = units // 4
    weights = (gate_weight, up_weight, down_weight)
    act_0, grads_0, down_0, back_0 = mlp(normed_mlp, cot_rows, *weights, 0, unit, (1, 2))
    pack_1, down_1, back_1 = mlp(normed_mlp, cot_rows, *weights, unit, unit, (3,))
    pack_2, down_2, back_2 = mlp(normed_mlp, cot_rows, *weights, 2 * unit, unit, (3,))
    pack_3, down_3, back_3 = mlp(normed_mlp, cot_rows, *weights, 3 * unit, unit, (3,))
    mlp_part = down_0 + down_1 + down_2 + down_3
    back_part = back_0 + back_1 + back_2 + back_3

    cot_cols = dp_columns(cot_rows)
    normed_cols = dp_columns(normed)
    attended_all = dp_rows(attended[None])
    nm_cols = dp_columns(normed_mlp)
    both = [cot_cols, nm_cols]
    act_0, grads_0 = dp_rows(act_0), dp_rows(grads_0)
    pack_1, pack_2 = dp_rows(pack_1), dp_rows(pack_2)
    pack_3 = dp_rows(pack_3)
    wg_0 = weight_grad(None, unit, 0, [cot_cols], (0,), act_0)
    wg_1 = weight_grad(None, 2 * unit, 0, [nm_cols], (0, 0), grads_0)
    wg_2 = weight_grad(None, 3 * unit, 0, both, (0, 1, 1), pack_1)
    wg_3 = weight_grad(None, 6 * unit, 0, both, (0, 1, 1), pack_2)
    wg_3 = weight_grad(wg_3, 6 * unit, 3 * unit, both, (0, 1, 1), pack_3)
    first_sum = ctx_scatter(wg_0)
    second_sum = ctx_scatter(wg_1)
    third_sum = ctx_scatter(wg_2)
    fourth_sum = ctx_scatter(wg_3)
    qkv_cols = query_cols + 2 * kv_cols
    total = qkv_cols + query_cols + 128

    hidden_deep = hidden.reshape(deep)
    block_out = (share_of(hidden_deep) + sum_share(mlp_part.reshape(deep))).astype(bf16)
    unit_second = hidden * r_second
    mlp_gain_part = jnp.sum(back_part * unit_second, axis=0)
    scaled = gain_second * sum_whole(back_part)
    grad_hidden = cot_rows.astype(f32) + r_second * (
        scaled - unit_second * jnp.mean(scaled * unit_second, axis=-1, keepdims=True)
    )
    grad_branch = grad_hidden.astype(bf16)
    grad_attended = dot_nt(grad_branch, output_weight).astype(bf16)
    branch_cols = dp_columns(grad_branch)
    last = weight_grad(None, total, qkv_cols, [branch_cols], (0,), attended_all)

    grad_query_raw, kv_sum, *kv_given = attend_back(
        queries, kv_blocks, grad_attended, cosine, sine, ctx_tok
    )
    for back, piece in enumerate(kv_given, 1):
        given = lax.ppermute(piece, "ctx", [(i + back, i) for i in range(ctx_ranks - back)])
        kv_sum = kv_sum + given.astype(f32)
    kv_sum = kv_sum.reshape(seq_count, ctx_tok, 2, kv_cols // HD, 2, HD // 2)
    first_half, second_half = kv_sum[..., 0, :], kv_sum[..., 1, :]
    cos_half = jnp.stack([cosine[:, : HD // 2], ones[:, : HD // 2]], axis=1)[:, :, None]
    sin_half = jnp.stack([sine[:, HD // 2 : HD], ones[:, : HD // 2] * 0.0], axis=1)[:, :, None]
    grad_kv_raw = (
        jnp.stack(
            [
                first_half * cos_half + second_half * sin_half,
                second_half * cos_half - first_half * sin_half,
            ],
            axis=-2,
        )
        .astype(bf16)
        .reshape(rows, 2 * kv_cols)
    )
    grad_raw = jnp.concatenate([grad_query_raw, grad_kv_raw], axis=1)
    raw_all = dp_rows(grad_raw[None])
    last = weight_grad(last, total, 0, [normed_cols], (0,), raw_all)
    grad_normed_first = (
        dot_nt(grad_query_raw, query_weight)
        + dot_nt(grad_kv_raw[:, :kv_cols], key_weight)
        + dot_nt(grad_kv_raw[:, kv_cols:], value_weight)
    )
    full_in = flat_in.astype(f32)
    r_first = lax.rsqrt(jnp.mean(full_in * full_in, axis=-1, keepdims=True) + norm_eps)
    unit_first = full_in * r_first
    attn_gain_part = jnp.sum(grad_normed_first * unit_first, axis=0)
    gains = gains_own(jnp.stack([attn_gain_part, mlp_gain_part]))
    gain_block = jnp.pad(gains.T.astype(bf16), ((0, 0), (0, 126)))
    last = lax.dynamic_update_slice(last, gain_block, (0, total - 128))
    last_sum = ctx_scatter(last)

    scaled_first = gain_first * sum_share(grad_normed_first.reshape(deep))
    unit_share = share_of(unit_first.reshape(deep))
    input_grad = share_of(grad_hidden.reshape(deep)) + share_of(r_first.reshape(seq_count, ctx_tok, 1)) * (
        scaled_first - unit_share * jnp.mean(scaled_first * unit_share, axis=-1, keepdims=True)
    )

    def joined(*parts):
        return jnp.concatenate(parts, axis=1).astype(f32)

    piece = lambda summed, at: summed[:, at * unit : (at + 1) * unit]
    grad_down = joined(first_sum, piece(third_sum, 0), piece(fourth_sum, 0), piece(fourth_sum, 3)).T
    grad_gate = joined(
        piece(second_sum, 0), piece(third_sum, 1), piece(fourth_sum, 1), piece(fourth_sum, 4)
    )
    grad_up = joined(
        piece(second_sum, 1), piece(third_sum, 2), piece(fourth_sum, 2), piece(fourth_sum, 5)
    )
    query_end = query_cols
    key_end = query_end + kv_cols
    value_end = key_end + kv_cols
    cut = lambda first, end: last_sum[:, first:end].astype(f32)
    gains_out = cut(total - 128, total - 126)
    return (
        block_out,
        input_grad,
        gains_out[:, 0],
        cut(0, query_end),
        cut(query_end, key_end),
        cut(key_end, value_end),
        cut(value_end, total - 128).T,
        gains_out[:, 1],
        grad_gate,
        grad_up,
        grad_down,
    )


def solution(mesh):
    in_specs = (
        P("dp", "ctx", None),
        P(),
        P(None, "tensor"),
        P(None, "tensor"),
        P(None, "tensor"),
        P("tensor", None),
        P(),
        P(None, "tensor"),
        P(None, "tensor"),
        P("tensor", None),
        P("dp", "ctx", None),
    )
    out_specs = (
        P("dp", ("ctx", "tensor"), None),
        P("dp", ("ctx", "tensor"), None),
        P(("dp", "ctx")),
        P(("dp", "ctx"), "tensor"),
        P(("dp", "ctx"), "tensor"),
        P(("dp", "ctx"), "tensor"),
        P("tensor", ("dp", "ctx")),
        P(("dp", "ctx")),
        P(("dp", "ctx"), "tensor"),
        P(("dp", "ctx"), "tensor"),
        P("tensor", ("dp", "ctx")),
    )

    return jax.shard_map(shards, mesh=mesh, in_specs=in_specs, out_specs=out_specs, check_vma=False)
```

```python
import jax
import jax.numpy as jnp
from jax import lax
from jax.experimental import pallas as pl
from jax.experimental.pallas import tpu as pltpu
from jax.sharding import PartitionSpec as P


HD = 64

norm_eps = 1e-05
rope_base = 500000.0
f32 = jnp.float32
bf16 = jnp.bfloat16


def rms_apply(values, gain):
    return values * lax.rsqrt(jnp.mean(values * values, axis=-1, keepdims=True) + norm_eps) * gain


def rope_tables(positions, head_size):
    half_width = head_size // 2
    frequency = rope_base ** (-jnp.arange(half_width, dtype=f32) * 2.0 / head_size)
    angles = positions.astype(f32)[:, None] * frequency[None, :]
    return (jnp.cos(angles)[:, None, :], jnp.sin(angles)[:, None, :])


def dot_nn(left, right):
    return lax.dot_general(left, right, (((1,), (0,)), ((), ())), preferred_element_type=f32)


def dot_tn(left, right):
    return lax.dot_general(left, right, (((0,), (0,)), ((), ())), preferred_element_type=f32)


def dot_nt(left, right):
    return lax.dot_general(left, right, (((1,), (1,)), ((), ())), preferred_element_type=f32)


def call(body, grid, in_specs, out_specs, out_shape, flops, moved, **rest):
    return pl.pallas_call(
        body,
        grid=grid,
        in_specs=in_specs,
        out_specs=out_specs,
        out_shape=out_shape,
        cost_estimate=pl.CostEstimate(flops=flops, bytes_accessed=moved, transcendentals=0),
        compiler_params=pltpu.CompilerParams(vmem_limit_bytes=56 << 20),
        **rest,
    )


def whole(shape):
    zeros = (0,) * len(shape)
    return pl.BlockSpec(shape, lambda *_: zeros, pipeline_mode=pl.Buffered(1))


def shape_of(shape, kind):
    return jax.ShapeDtypeStruct(shape, kind)


def turned(values, cosine, sine):
    at = lax.broadcasted_iota(jnp.int32, values.shape, 1) % HD
    swapped = jnp.where(
        at < HD // 2, pltpu.roll(values, 128 - HD // 2, 1), pltpu.roll(values, HD // 2, 1)
    )
    return values * cosine + swapped * sine


def rope_columns(positions):
    cosine, sine = rope_tables(positions, HD)
    cosine, sine = cosine[:, 0], sine[:, 0]
    return jnp.tile(cosine, (1, 4)), jnp.tile(jnp.concatenate([-sine, sine], axis=-1), (1, 2))


def norm_kv(rows, gain, key_weight, value_weight, cosine, sine):
    count, width = rows.shape
    cols = key_weight.shape[1]
    tokens = cosine.shape[0]

    def body(rows_ref, gain_ref, key_ref, value_ref, cos_ref, sin_ref, normed_ref, kv_ref):
        values = rows_ref[...].astype(f32)
        normed = rms_apply(values, gain_ref[...].astype(f32)).astype(bf16)
        normed_ref[...] = normed
        raw = jnp.concatenate([dot_nn(normed, key_ref[...]), dot_nn(normed, value_ref[...])], axis=1)
        for first in range(0, count, tokens):
            for at in range(0, 2 * cols, 128):
                part = raw[first : first + tokens, at : at + 128]
                kv_ref[first : first + tokens, at : at + 128] = turned(
                    part, cos_ref[:, at : at + 128], sin_ref[:, at : at + 128]
                ).astype(bf16)

    shapes = [rows.shape, gain.shape, key_weight.shape, value_weight.shape, cosine.shape, sine.shape]
    return call(
        body,
        (1,),
        [whole(s) for s in shapes],
        [whole(rows.shape), whole((count, 2 * cols))],
        [shape_of(rows.shape, bf16), shape_of((count, 2 * cols), bf16)],
        4 * count * width * cols,
        2 * (2 * count * width + 2 * width * cols),
    )(rows, gain, key_weight, value_weight, cosine, sine)


def tile_of(*sizes):
    for tile in (512, 256, 128):
        if all(size % tile == 0 for size in sizes):
            return tile
    raise ValueError("no tile")


def project_queries(normed, weight, cosine, sine):
    count, width = normed.shape
    cols = weight.shape[1]
    tokens = cosine.shape[0]
    tile = tile_of(cols)

    def body(normed_ref, weight_ref, cos_ref, sin_ref, out_ref):
        raw = dot_nn(normed_ref[...], weight_ref[...])
        for first in range(0, count, tokens):
            for at in range(0, tile, 128):
                out_ref[first : first + tokens, at : at + 128] = turned(
                    raw[first : first + tokens, at : at + 128], cos_ref[...], sin_ref[...]
                ).astype(bf16)

    return call(
        body,
        (cols // tile,),
        [
            whole(normed.shape),
            pl.BlockSpec((width, tile), lambda i: (0, i)),
            whole(cosine.shape),
            whole(sine.shape),
        ],
        pl.BlockSpec((count, tile), lambda i: (0, i)),
        shape_of((count, cols), bf16),
        2 * count * width * cols,
        2 * (count * width + width * cols),
    )(normed, weight, cosine, sine)


def scores_of(stacked, keys, ctx_at, scale):
    tokens = keys[0].shape[0]
    found = []
    for back, block in enumerate(keys):
        raw = dot_nt(stacked, block) * scale
        if back == 0:
            query_at = lax.broadcasted_iota(jnp.int32, raw.shape, 0) % tokens
            seen = query_at >= lax.broadcasted_iota(jnp.int32, raw.shape, 1)
            found.append(jnp.where(seen, raw, -1e30))
        else:
            found.append(raw + jnp.where(ctx_at >= back, 0.0, -1e30).astype(f32))
    most = jnp.max(found[0], axis=-1, keepdims=True)
    for masked in found[1:]:
        most = jnp.maximum(most, jnp.max(masked, axis=-1, keepdims=True))
    found = [jnp.exp(masked - most) for masked in found]
    total = sum(jnp.sum(part, axis=-1, keepdims=True) for part in found)
    inverse = 1.0 / total
    return [part * inverse for part in found]


def stack_heads(ref, head, group):
    first = head * group
    return jnp.concatenate(
        [ref[:, (first + g) * HD : (first + g + 1) * HD] for g in range(group)], axis=0
    )


def attend(queries, kv_blocks, tokens):
    count, cols = queries.shape
    kv_cols = kv_blocks[0].shape[1] // 2
    heads = kv_cols // HD
    group = cols // kv_cols
    scale = HD ** (-0.5)
    blocks = len(kv_blocks)

    def body(query_ref, *refs):
        out_ref = refs[-1]
        ctx_at = lax.axis_index("ctx")
        for head in range(heads):
            stacked = stack_heads(query_ref, head, group)
            at = head * HD
            keys = [ref[:, at : at + HD] for ref in refs[:blocks]]
            probs = scores_of(stacked, keys, ctx_at, scale)
            total = sum(
                dot_nn(part.astype(bf16), ref[:, kv_cols + at : kv_cols + at + HD])
                for part, ref in zip(probs, refs)
            )
            for g in range(group):
                first = (head * group + g) * HD
                out_ref[:, first : first + HD] = total[g * tokens : (g + 1) * tokens].astype(bf16)

    rows = lambda width: pl.BlockSpec((tokens, width), lambda i: (i, 0))
    return call(
        body,
        (count // tokens,),
        [rows(cols)] + [rows(2 * kv_cols)] * blocks,
        rows(cols),
        shape_of((count, cols), bf16),
        40 * count * cols * tokens * blocks,
        2 * count * (2 * cols + 2 * kv_cols * blocks),
    )(queries, *kv_blocks)


def attend_back(queries, kv_blocks, grad_attended, cosine, sine, tokens):
    count, cols = queries.shape
    kv_cols = kv_blocks[0].shape[1] // 2
    heads = kv_cols // HD
    group = cols // kv_cols
    scale = HD ** (-0.5)
    blocks = len(kv_blocks)

    def body(query_ref, grad_ref, cos_ref, sin_ref, *refs):
        kv_refs, query_out, kv_out = refs[:blocks], refs[blocks], refs[blocks + 1 : -1]
        turned_ref = refs[-1]
        ctx_at = lax.axis_index("ctx")
        for head in range(heads):
            stacked = stack_heads(query_ref, head, group)
            grads = stack_heads(grad_ref, head, group)
            at = head * HD
            keys = [ref[:, at : at + HD] for ref in kv_refs]
            values = [ref[:, kv_cols + at : kv_cols + at + HD] for ref in kv_refs]
            probs = scores_of(stacked, keys, ctx_at, scale)
            grad_probs = [dot_nt(grads, block) for block in values]
            inner = sum(
                jnp.sum(part * grad, axis=-1, keepdims=True)
                for part, grad in zip(probs, grad_probs)
            )
            total = 0.0
            for back in range(blocks):
                grad_scores = (probs[back] * (grad_probs[back] - inner)).astype(bf16)
                total = total + dot_nn(grad_scores, keys[back])
                kind = kv_out[back].dtype
                kv_out[back][:, at : at + HD] = (dot_tn(grad_scores, stacked) * scale).astype(kind)
                kv_out[back][:, kv_cols + at : kv_cols + at + HD] = dot_tn(
                    probs[back].astype(bf16), grads
                ).astype(kind)
            for g in range(group):
                first = (head * group + g) * HD
                turned_ref[:, first : first + HD] = total[g * tokens : (g + 1) * tokens] * scale
        for at in range(0, cols, 128):
            query_out[:, at : at + 128] = turned(
                turned_ref[:, at : at + 128], cos_ref[...], -sin_ref[...]
            ).astype(bf16)

    rows = lambda width: pl.BlockSpec((tokens, width), lambda i: (i, 0))
    return call(
        body,
        (count // tokens,),
        [rows(cols), rows(cols), whole(cosine.shape), whole(sine.shape)]
        + [rows(2 * kv_cols)] * blocks,
        [rows(cols)] + [rows(2 * kv_cols)] * blocks,
        [shape_of((count, cols), bf16)]
        + [shape_of((count, 2 * kv_cols), f32 if back == 0 else bf16) for back in range(blocks)],
        100 * count * cols * tokens * blocks,
        2 * count * (3 * cols + 4 * kv_cols * blocks),
        scratch_shapes=[pltpu.VMEM((tokens, cols), f32)],
    )(queries, grad_attended, cosine, sine, *kv_blocks)


def mlp(normed, cot, gate_weight, up_weight, down_weight, start, size, parts):
    count, width = normed.shape
    tile = tile_of(start, size)
    base = start // tile

    def body(normed_ref, cot_ref, gate_ref, up_ref, down_ref, *refs):
        out_refs, down_sum, back_sum = refs[:-2], refs[-2], refs[-1]
        gate = dot_nn(normed_ref[...], gate_ref[...])
        up = dot_nn(normed_ref[...], up_ref[...])
        grad = dot_nt(cot_ref[...], down_ref[...])
        sig = 1.0 / (1.0 + jnp.exp(-gate))
        silu = gate * sig
        activated = (silu * up).astype(bf16)
        grad_gate = (grad * up * sig * (1.0 + gate * (1.0 - sig))).astype(bf16)
        grad_up = (grad * silu).astype(bf16)
        made = [activated, grad_gate, grad_up]
        at = 0
        for ref in out_refs:
            for i in range(ref.shape[0]):
                ref[i] = made[at]
                at += 1
        first = pl.program_id(0) == 0

        @pl.when(first)
        def _():
            down_sum[...] = dot_nn(activated, down_ref[...])
            back_sum[...] = dot_nt(grad_gate, gate_ref[...]) + dot_nt(grad_up, up_ref[...])

        @pl.when(jnp.logical_not(first))
        def _():
            down_sum[...] += dot_nn(activated, down_ref[...])
            back_sum[...] += dot_nt(grad_gate, gate_ref[...]) + dot_nt(grad_up, up_ref[...])

    held = whole((count, width))
    columns = pl.BlockSpec((width, tile), lambda i: (0, base + i))
    return call(
        body,
        (size // tile,),
        [held, held, columns, columns, pl.BlockSpec((tile, width), lambda i: (base + i, 0))],
        [pl.BlockSpec((n, count, tile), lambda i: (0, 0, i)) for n in parts] + [held, held],
        [shape_of((n, count, size), bf16) for n in parts]
        + [shape_of((count, width), f32)] * 2,
        12 * count * width * size,
        2 * (3 * width * size + 3 * count * size + 6 * count * width),
    )(normed, cot, gate_weight, up_weight, down_weight)


def weight_grad(buffer, total, start, lefts, chosen, rights):
    entries, count, size = rights[0].shape
    own = lefts[0][0].shape[1]
    tile = tile_of(start, size)
    base, steps = start // tile, size // tile
    sources = len(rights)
    given = 0 if buffer is None else 1

    def body(*refs):
        out_ref = refs[-1]
        rights_at = refs[given + sources * len(lefts) : -1]

        def product(which):
            left = refs[given + sources * which : given + sources * (which + 1)]
            out_ref[...] = sum(dot_tn(a[...], b[0]) for a, b in zip(left, rights_at)).astype(bf16)

        for which in range(len(lefts)):
            if len(lefts) == 1:
                product(0)
            else:
                mine = [v for v in range(entries) if chosen[v] == which]
                v = pl.program_id(0)
                pl.when((v >= mine[0]) & (v <= mine[-1]))(lambda which=which: product(which))

    return call(
        body,
        (entries, steps),
        [pl.BlockSpec(memory_space=pl.ANY)] * given
        + [whole((count, own))] * (sources * len(lefts))
        + [pl.BlockSpec((1, count, tile), lambda v, i: (v, 0, i))] * sources,
        pl.BlockSpec((own, tile), lambda v, i: (0, base + v * steps + i)),
        shape_of((own, total), bf16),
        2 * entries * sources * count * own * size,
        2 * entries * size * (sources * count + own),
        input_output_aliases={0: 0} if given else {},
    )(*([] if buffer is None else [buffer]), *(p for left in lefts for p in left), *rights)


def xor_pairs(count, bit):
    return [(i, i ^ bit) for i in range(count)]


def dp_bits():
    count = lax.axis_size("dp")
    bits = []
    bit = count // 2
    while bit:
        bits.append(bit)
        bit //= 2
    return count, bits


def moved_dp(parts, bit):
    found = []
    for part in parts:
        found.append(lax.ppermute(part, "dp", xor_pairs(lax.axis_size("dp"), bit)))
    return found


def dp_rows(rows):
    _, bits = dp_bits()
    found = [rows]
    for bit in bits:
        found = found + moved_dp(found, bit)
    return found


def dp_columns(rows):
    _, bits = dp_bits()
    me = lax.axis_index("dp")
    found = [rows]
    for bit in bits:
        half = found[0].shape[1] // 2
        upper = (me // bit) % 2
        keep = [lax.dynamic_slice_in_dim(part, upper * half, half, 1) for part in found]
        give = [lax.dynamic_slice_in_dim(part, (1 - upper) * half, half, 1) for part in found]
        found = keep + moved_dp(give, bit)
    return found


def swap_tensor(values):
    return lax.ppermute(values, "tensor", [(0, 1), (1, 0)])


def sum_share(part):
    ranks = lax.axis_size("tensor")
    if ranks != 2:
        return lax.psum_scatter(part.astype(bf16), "tensor", scatter_dimension=1, tiled=True).astype(f32)
    share = part.shape[1] // 2
    me = lax.axis_index("tensor")
    mine = lax.dynamic_slice_in_dim(part, me * share, share, 1)
    theirs = lax.dynamic_slice_in_dim(part, (1 - me) * share, share, 1)
    return mine + swap_tensor(theirs.astype(bf16)).astype(f32)


def sum_whole(part):
    if lax.axis_size("tensor") != 2:
        return lax.psum(part.astype(bf16), "tensor").astype(f32)
    low = part.astype(bf16)
    return low.astype(f32) + swap_tensor(low).astype(f32)


def other_weight(weight):
    count, _ = dp_bits()
    size = weight.shape[0] // count
    own = lax.dynamic_slice_in_dim(weight, lax.axis_index("dp") * size, size, 0)
    return dp_rows(swap_tensor(own))


def join_branch(base, theirs, pieces, gain):
    count, width = base.shape
    size = pieces[0].shape[0]
    order = [0]
    for bit in dp_bits()[1]:
        order = order + [at ^ bit for at in order]

    def body(base_ref, theirs_ref, gain_ref, *refs):
        piece_refs, (hidden_ref, scale_ref, normed_ref) = refs[:-3], refs[-3:]
        me = lax.axis_index("dp")
        total = base_ref[...]
        for flip, ref in zip(order, piece_refs):
            at = pl.multiple_of((me ^ flip) * size, size)
            total = total + dot_nn(theirs_ref[:, pl.ds(at, size)], ref[...])
        hidden_ref[...] = total
        scale = lax.rsqrt(jnp.mean(total * total, axis=-1, keepdims=True) + norm_eps)
        scale_ref[...] = scale
        normed_ref[...] = (total * scale * gain_ref[...].astype(f32)).astype(bf16)

    return call(
        body,
        (1,),
        [whole(base.shape), whole(theirs.shape), whole(gain.shape)] + [whole(p.shape) for p in pieces],
        [whole(base.shape), whole((count, 1)), whole(base.shape)],
        [shape_of(base.shape, f32), shape_of((count, 1), f32), shape_of(base.shape, bf16)],
        2 * count * width * size * len(pieces),
        2 * (5 * count * width + width * size * len(pieces)),
    )(base, theirs, gain, *pieces)


def ctx_scatter(block):
    return lax.psum_scatter(block, "ctx", scatter_dimension=0, tiled=True)


def ctx_ring(block):
    count = lax.axis_size("ctx")
    me = lax.axis_index("ctx")
    size = block.shape[0] // count

    def part(back):
        at = (me - back + count) % count
        return lax.dynamic_slice_in_dim(block, at * size, size, 0)

    total = part(1)
    for step in range(count - 1):
        moved = lax.ppermute(total, "ctx", [(i, (i + 1) % count) for i in range(count)])
        total = (moved.astype(f32) + part(step + 2).astype(f32)).astype(bf16)
    return total


def gains_own(parts):
    if lax.axis_size("tensor") == 2:
        parts = parts + swap_tensor(parts)
    else:
        parts = lax.psum(parts, "tensor")
    count, bits = dp_bits()
    me = lax.axis_index("dp")
    for bit in bits:
        half = parts.shape[1] // 2
        upper = (me // bit) % 2
        keep = lax.dynamic_slice_in_dim(parts, upper * half, half, 1)
        give = lax.dynamic_slice_in_dim(parts, (1 - upper) * half, half, 1)
        parts = keep + lax.ppermute(give, "dp", xor_pairs(count, bit))
    return parts


def shards(
    block_in,
    attn_gain,
    query_weight,
    key_weight,
    value_weight,
    output_weight,
    mlp_gain,
    gate_weight,
    up_weight,
    down_weight,
    cotangent,
):
    seq_count, ctx_tok, width = block_in.shape
    ctx_ranks = lax.axis_size("ctx")
    tensor_ranks = lax.axis_size("tensor")
    share_len = ctx_tok // tensor_ranks
    share_start = lax.axis_index("tensor") * share_len
    rows = seq_count * ctx_tok
    query_cols = query_weight.shape[1]
    kv_cols = key_weight.shape[1]
    units = gate_weight.shape[1]
    ctx_at = lax.axis_index("ctx")
    deep = (seq_count, ctx_tok, width)

    def share_of(values):
        return lax.dynamic_slice_in_dim(values, share_start, share_len, 1)

    gain_first = attn_gain.astype(f32)
    gain_second = mlp_gain.astype(f32)
    flat_in = block_in.reshape(rows, width)
    cot_rows = cotangent.reshape(rows, width)
    positions = ctx_at * ctx_tok + jnp.arange(ctx_tok, dtype=jnp.int32)
    cosine, sine = rope_columns(positions)
    ones = jnp.ones((ctx_tok, kv_cols), f32)
    table = lambda one, rest: jnp.concatenate(
        [jnp.tile(one[:, :HD], (1, kv_cols // HD)), rest], axis=1
    )
    kv_cosine, kv_sine = table(cosine, ones), table(sine, ones * 0.0)

    normed, kv_own = norm_kv(flat_in, attn_gain[None], key_weight, value_weight, kv_cosine, kv_sine)
    kv_blocks = [kv_own]
    for back in range(1, ctx_ranks):
        kv_blocks.append(
            lax.ppermute(kv_own, "ctx", [(i, i + back) for i in range(ctx_ranks - back)])
        )
    queries = project_queries(normed, query_weight, cosine, sine)
    attended = attend(queries, kv_blocks, ctx_tok)
    branch = dot_nn(attended, output_weight)
    if tensor_ranks == 2:
        theirs = swap_tensor(attended)
        pieces = other_weight(output_weight)
        hidden, r_second, normed_mlp = join_branch(
            flat_in.astype(f32) + branch, theirs, pieces, mlp_gain[None]
        )
    else:
        hidden = flat_in.astype(f32) + lax.psum(branch, "tensor")
        r_second = lax.rsqrt(jnp.mean(hidden * hidden, axis=-1, keepdims=True) + norm_eps)
        normed_mlp = (hidden * r_second * gain_second).astype(bf16)

    unit = units // 4
    weights = (gate_weight, up_weight, down_weight)
    act_0, grads_0, down_0, back_0 = mlp(normed_mlp, cot_rows, *weights, 0, unit, (1, 2))
    pack_1, down_1, back_1 = mlp(normed_mlp, cot_rows, *weights, unit, unit, (3,))
    pack_2, down_2, back_2 = mlp(normed_mlp, cot_rows, *weights, 2 * unit, unit, (3,))
    pack_3, down_3, back_3 = mlp(normed_mlp, cot_rows, *weights, 3 * unit, unit, (3,))
    mlp_part = down_0 + down_1 + down_2 + down_3
    back_part = back_0 + back_1 + back_2 + back_3

    cot_cols = dp_columns(cot_rows)
    normed_cols = dp_columns(normed)
    attended_all = dp_rows(attended[None])
    nm_cols = dp_columns(normed_mlp)
    both = [cot_cols, nm_cols]
    act_0, grads_0 = dp_rows(act_0), dp_rows(grads_0)
    pack_1, pack_2 = dp_rows(pack_1), dp_rows(pack_2)
    pack_3 = dp_rows(pack_3)
    wg_0 = weight_grad(None, unit, 0, [cot_cols], (0,), act_0)
    wg_1 = weight_grad(None, 2 * unit, 0, [nm_cols], (0, 0), grads_0)
    wg_2 = weight_grad(None, 3 * unit, 0, both, (0, 1, 1), pack_1)
    wg_3 = weight_grad(None, 3 * unit, 0, both, (0, 1, 1), pack_2)
    wg_4 = weight_grad(None, 3 * unit, 0, both, (0, 1, 1), pack_3)
    first_sum = ctx_scatter(wg_0)
    second_sum = ctx_scatter(wg_1)
    third_sum = ctx_scatter(wg_2)
    ring_sum = ctx_ring(wg_3)
    fourth_sum = ctx_scatter(wg_4)
    qkv_cols = query_cols + 2 * kv_cols
    total = qkv_cols + query_cols + 128

    hidden_deep = hidden.reshape(deep)
    block_out = (share_of(hidden_deep) + sum_share(mlp_part.reshape(deep))).astype(bf16)
    unit_second = hidden * r_second
    mlp_gain_part = jnp.sum(back_part * unit_second, axis=0)
    scaled = gain_second * sum_whole(back_part)
    grad_hidden = cot_rows.astype(f32) + r_second * (
        scaled - unit_second * jnp.mean(scaled * unit_second, axis=-1, keepdims=True)
    )
    grad_branch = grad_hidden.astype(bf16)
    grad_attended = dot_nt(grad_branch, output_weight).astype(bf16)
    branch_cols = dp_columns(grad_branch)
    last = weight_grad(None, total, qkv_cols, [branch_cols], (0,), attended_all)

    grad_query_raw, kv_sum, *kv_given = attend_back(
        queries, kv_blocks, grad_attended, cosine, sine, ctx_tok
    )
    for back, piece in enumerate(kv_given, 1):
        given = lax.ppermute(piece, "ctx", [(i + back, i) for i in range(ctx_ranks - back)])
        kv_sum = kv_sum + given.astype(f32)
    kv_sum = kv_sum.reshape(seq_count, ctx_tok, 2, kv_cols // HD, 2, HD // 2)
    first_half, second_half = kv_sum[..., 0, :], kv_sum[..., 1, :]
    cos_half = jnp.stack([cosine[:, : HD // 2], ones[:, : HD // 2]], axis=1)[:, :, None]
    sin_half = jnp.stack([sine[:, HD // 2 : HD], ones[:, : HD // 2] * 0.0], axis=1)[:, :, None]
    grad_kv_raw = (
        jnp.stack(
            [
                first_half * cos_half + second_half * sin_half,
                second_half * cos_half - first_half * sin_half,
            ],
            axis=-2,
        )
        .astype(bf16)
        .reshape(rows, 2 * kv_cols)
    )
    grad_raw = jnp.concatenate([grad_query_raw, grad_kv_raw], axis=1)
    raw_all = dp_rows(grad_raw[None])
    last = weight_grad(last, total, 0, [normed_cols], (0,), raw_all)
    grad_normed_first = (
        dot_nt(grad_query_raw, query_weight)
        + dot_nt(grad_kv_raw[:, :kv_cols], key_weight)
        + dot_nt(grad_kv_raw[:, kv_cols:], value_weight)
    )
    full_in = flat_in.astype(f32)
    r_first = lax.rsqrt(jnp.mean(full_in * full_in, axis=-1, keepdims=True) + norm_eps)
    unit_first = full_in * r_first
    attn_gain_part = jnp.sum(grad_normed_first * unit_first, axis=0)
    gains = gains_own(jnp.stack([attn_gain_part, mlp_gain_part]))
    gain_block = jnp.pad(gains.T.astype(bf16), ((0, 0), (0, 126)))
    last = lax.dynamic_update_slice(last, gain_block, (0, total - 128))
    last_sum = ctx_scatter(last)

    scaled_first = gain_first * sum_share(grad_normed_first.reshape(deep))
    unit_share = share_of(unit_first.reshape(deep))
    input_grad = share_of(grad_hidden.reshape(deep)) + share_of(r_first.reshape(seq_count, ctx_tok, 1)) * (
        scaled_first - unit_share * jnp.mean(scaled_first * unit_share, axis=-1, keepdims=True)
    )

    def joined(*parts):
        return jnp.concatenate(parts, axis=1).astype(f32)

    piece = lambda summed, at: summed[:, at * unit : (at + 1) * unit]
    grad_down = joined(first_sum, piece(third_sum, 0), piece(ring_sum, 0), piece(fourth_sum, 0)).T
    grad_gate = joined(
        piece(second_sum, 0), piece(third_sum, 1), piece(ring_sum, 1), piece(fourth_sum, 1)
    )
    grad_up = joined(
        piece(second_sum, 1), piece(third_sum, 2), piece(ring_sum, 2), piece(fourth_sum, 2)
    )
    query_end = query_cols
    key_end = query_end + kv_cols
    value_end = key_end + kv_cols
    cut = lambda first, end: last_sum[:, first:end].astype(f32)
    gains_out = cut(total - 128, total - 126)
    return (
        block_out,
        input_grad,
        gains_out[:, 0],
        cut(0, query_end),
        cut(query_end, key_end),
        cut(key_end, value_end),
        cut(value_end, total - 128).T,
        gains_out[:, 1],
        grad_gate,
        grad_up,
        grad_down,
    )


def solution(mesh):
    in_specs = (
        P("dp", "ctx", None),
        P(),
        P(None, "tensor"),
        P(None, "tensor"),
        P(None, "tensor"),
        P("tensor", None),
        P(),
        P(None, "tensor"),
        P(None, "tensor"),
        P("tensor", None),
        P("dp", "ctx", None),
    )
    out_specs = (
        P("dp", ("ctx", "tensor"), None),
        P("dp", ("ctx", "tensor"), None),
        P(("dp", "ctx")),
        P(("dp", "ctx"), "tensor"),
        P(("dp", "ctx"), "tensor"),
        P(("dp", "ctx"), "tensor"),
        P("tensor", ("dp", "ctx")),
        P(("dp", "ctx")),
        P(("dp", "ctx"), "tensor"),
        P(("dp", "ctx"), "tensor"),
        P("tensor", ("dp", "ctx")),
    )

    return jax.shard_map(shards, mesh=mesh, in_specs=in_specs, out_specs=out_specs, check_vma=False)
```

```python
import jax
import jax.numpy as jnp
from jax import lax
from jax.experimental import pallas as pl
from jax.experimental.pallas import tpu as pltpu
from jax.sharding import PartitionSpec as P


HD = 64

norm_eps = 1e-05
rope_base = 500000.0
f32 = jnp.float32
bf16 = jnp.bfloat16


def rms_apply(values, gain):
    return values * lax.rsqrt(jnp.mean(values * values, axis=-1, keepdims=True) + norm_eps) * gain


def rope_tables(positions, head_size):
    half_width = head_size // 2
    frequency = rope_base ** (-jnp.arange(half_width, dtype=f32) * 2.0 / head_size)
    angles = positions.astype(f32)[:, None] * frequency[None, :]
    return (jnp.cos(angles)[:, None, :], jnp.sin(angles)[:, None, :])


def dot_nn(left, right):
    return lax.dot_general(left, right, (((1,), (0,)), ((), ())), preferred_element_type=f32)


def dot_tn(left, right):
    return lax.dot_general(left, right, (((0,), (0,)), ((), ())), preferred_element_type=f32)


def dot_nt(left, right):
    return lax.dot_general(left, right, (((1,), (1,)), ((), ())), preferred_element_type=f32)


def call(body, grid, in_specs, out_specs, out_shape, flops, moved, **rest):
    return pl.pallas_call(
        body,
        grid=grid,
        in_specs=in_specs,
        out_specs=out_specs,
        out_shape=out_shape,
        cost_estimate=pl.CostEstimate(flops=flops, bytes_accessed=moved, transcendentals=0),
        compiler_params=pltpu.CompilerParams(vmem_limit_bytes=56 << 20),
        **rest,
    )


def whole(shape):
    zeros = (0,) * len(shape)
    return pl.BlockSpec(shape, lambda *_: zeros, pipeline_mode=pl.Buffered(1))


def shape_of(shape, kind):
    return jax.ShapeDtypeStruct(shape, kind)


def turned(values, cosine, sine):
    at = lax.broadcasted_iota(jnp.int32, values.shape, 1) % HD
    swapped = jnp.where(
        at < HD // 2, pltpu.roll(values, 128 - HD // 2, 1), pltpu.roll(values, HD // 2, 1)
    )
    return values * cosine + swapped * sine


def rope_columns(positions):
    cosine, sine = rope_tables(positions, HD)
    cosine, sine = cosine[:, 0], sine[:, 0]
    return jnp.tile(cosine, (1, 4)), jnp.tile(jnp.concatenate([-sine, sine], axis=-1), (1, 2))


def norm_kv(rows, gain, key_weight, value_weight, cosine, sine):
    count, width = rows.shape
    cols = key_weight.shape[1]
    tokens = cosine.shape[0]

    def body(rows_ref, gain_ref, key_ref, value_ref, cos_ref, sin_ref, normed_ref, kv_ref):
        values = rows_ref[...].astype(f32)
        normed = rms_apply(values, gain_ref[...].astype(f32)).astype(bf16)
        normed_ref[...] = normed
        raw = jnp.concatenate([dot_nn(normed, key_ref[...]), dot_nn(normed, value_ref[...])], axis=1)
        for first in range(0, count, tokens):
            for at in range(0, 2 * cols, 128):
                part = raw[first : first + tokens, at : at + 128]
                kv_ref[first : first + tokens, at : at + 128] = turned(
                    part, cos_ref[:, at : at + 128], sin_ref[:, at : at + 128]
                ).astype(bf16)

    shapes = [rows.shape, gain.shape, key_weight.shape, value_weight.shape, cosine.shape, sine.shape]
    return call(
        body,
        (1,),
        [whole(s) for s in shapes],
        [whole(rows.shape), whole((count, 2 * cols))],
        [shape_of(rows.shape, bf16), shape_of((count, 2 * cols), bf16)],
        4 * count * width * cols,
        2 * (2 * count * width + 2 * width * cols),
    )(rows, gain, key_weight, value_weight, cosine, sine)


def tile_of(*sizes):
    for tile in (512, 256, 128):
        if all(size % tile == 0 for size in sizes):
            return tile
    raise ValueError("no tile")


def project_queries(normed, weight, cosine, sine):
    count, width = normed.shape
    cols = weight.shape[1]
    tokens = cosine.shape[0]
    tile = tile_of(cols)

    def body(normed_ref, weight_ref, cos_ref, sin_ref, out_ref):
        raw = dot_nn(normed_ref[...], weight_ref[...])
        for first in range(0, count, tokens):
            for at in range(0, tile, 128):
                out_ref[first : first + tokens, at : at + 128] = turned(
                    raw[first : first + tokens, at : at + 128], cos_ref[...], sin_ref[...]
                ).astype(bf16)

    return call(
        body,
        (cols // tile,),
        [
            whole(normed.shape),
            pl.BlockSpec((width, tile), lambda i: (0, i)),
            whole(cosine.shape),
            whole(sine.shape),
        ],
        pl.BlockSpec((count, tile), lambda i: (0, i)),
        shape_of((count, cols), bf16),
        2 * count * width * cols,
        2 * (count * width + width * cols),
    )(normed, weight, cosine, sine)


def probs_of(stacked, keys, tokens, ctx_at, scale):
    raw = dot_nt(stacked, keys) * scale
    found = []
    for back in range(keys.shape[0] // tokens):
        part = raw[:, back * tokens : (back + 1) * tokens]
        if back == 0:
            query_at = lax.broadcasted_iota(jnp.int32, part.shape, 0) % tokens
            seen = query_at >= lax.broadcasted_iota(jnp.int32, part.shape, 1)
            found.append(jnp.where(seen, part, -1e30))
        else:
            found.append(part + jnp.where(ctx_at >= back, 0.0, -1e30).astype(f32))
    most = found[0]
    for part in found[1:]:
        most = jnp.maximum(most, part)
    most = jnp.max(most, axis=-1, keepdims=True)
    found = [jnp.exp(part - most) for part in found]
    inverse = 1.0 / jnp.sum(sum(found), axis=-1, keepdims=True)
    return jnp.concatenate([part * inverse for part in found], axis=1)


def stack_heads(ref, head, group):
    first = head * group
    return jnp.concatenate(
        [ref[:, (first + g) * HD : (first + g + 1) * HD] for g in range(group)], axis=0
    )


def attend(queries, kv_blocks, tokens, seq):
    _, cols = queries.shape
    kv_cols = kv_blocks[0].shape[1] // 2
    heads = kv_cols // HD
    group = cols // kv_cols
    scale = HD ** (-0.5)
    blocks = len(kv_blocks)

    def body(query_ref, *refs):
        out_ref = refs[-1]
        ctx_at = lax.axis_index("ctx")
        for head in range(heads):
            stacked = stack_heads(query_ref, head, group)
            at = head * HD
            keys = jnp.concatenate([ref[:, at : at + HD] for ref in refs[:blocks]], axis=0)
            at += kv_cols
            values = jnp.concatenate([ref[:, at : at + HD] for ref in refs[:blocks]], axis=0)
            probs = probs_of(stacked, keys, tokens, ctx_at, scale)
            total = dot_nn(probs.astype(bf16), values)
            for g in range(group):
                first = (head * group + g) * HD
                out_ref[:, first : first + HD] = total[g * tokens : (g + 1) * tokens].astype(bf16)

    rows = lambda width: pl.BlockSpec((tokens, width), lambda i: (seq, 0))
    return call(
        body,
        (1,),
        [rows(cols)] + [rows(2 * kv_cols)] * blocks,
        whole((tokens, cols)),
        shape_of((tokens, cols), bf16),
        40 * tokens * cols * tokens * blocks,
        2 * tokens * (2 * cols + 2 * kv_cols * blocks),
    )(queries, *kv_blocks)


def attend_back(queries, kv_blocks, grad_attended, cosine, sine, tokens):
    count, cols = queries.shape
    kv_cols = kv_blocks[0].shape[1] // 2
    heads = kv_cols // HD
    group = cols // kv_cols
    scale = HD ** (-0.5)
    blocks = len(kv_blocks)

    def body(query_ref, grad_ref, cos_ref, sin_ref, *refs):
        kv_refs, query_out, kv_out = refs[:blocks], refs[blocks], refs[blocks + 1 : -1]
        turned_ref = refs[-1]
        ctx_at = lax.axis_index("ctx")
        for head in range(heads):
            stacked = stack_heads(query_ref, head, group)
            grads = stack_heads(grad_ref, head, group)
            at = head * HD
            keys = jnp.concatenate([ref[:, at : at + HD] for ref in kv_refs], axis=0)
            end = kv_cols + at
            values = jnp.concatenate([ref[:, end : end + HD] for ref in kv_refs], axis=0)
            probs = probs_of(stacked, keys, tokens, ctx_at, scale)
            grad_probs = dot_nt(grads, values)
            inner = jnp.sum(probs * grad_probs, axis=-1, keepdims=True)
            grad_scores = (probs * (grad_probs - inner)).astype(bf16)
            total = dot_nn(grad_scores, keys)
            grad_keys = dot_tn(grad_scores, stacked) * scale
            grad_values = dot_tn(probs.astype(bf16), grads)
            for back, ref in enumerate(kv_out):
                mine = slice(back * tokens, (back + 1) * tokens)
                ref[:, at : at + HD] = grad_keys[mine].astype(ref.dtype)
                ref[:, end : end + HD] = grad_values[mine].astype(ref.dtype)
            for g in range(group):
                first = (head * group + g) * HD
                turned_ref[:, first : first + HD] = total[g * tokens : (g + 1) * tokens] * scale
        for at in range(0, cols, 128):
            query_out[:, at : at + 128] = turned(
                turned_ref[:, at : at + 128], cos_ref[...], -sin_ref[...]
            ).astype(bf16)

    rows = lambda width: pl.BlockSpec((tokens, width), lambda i: (i, 0))
    return call(
        body,
        (count // tokens,),
        [rows(cols), rows(cols), whole(cosine.shape), whole(sine.shape)]
        + [rows(2 * kv_cols)] * blocks,
        [rows(cols)] + [rows(2 * kv_cols)] * blocks,
        [shape_of((count, cols), bf16)]
        + [shape_of((count, 2 * kv_cols), f32 if back == 0 else bf16) for back in range(blocks)],
        100 * count * cols * tokens * blocks,
        2 * count * (3 * cols + 4 * kv_cols * blocks),
        scratch_shapes=[pltpu.VMEM((tokens, cols), f32)],
    )(queries, grad_attended, cosine, sine, *kv_blocks)


def mlp(normed, cot, gate_weight, up_weight, down_weight, start, size, parts, packs=1):
    count, width = normed.shape
    tile = tile_of(start, size // packs)
    base = start // tile
    steps = size // packs // tile

    def body(normed_ref, cot_ref, gate_ref, up_ref, down_ref, *refs):
        out_refs, down_sum, back_sum = refs[:-2], refs[-2], refs[-1]
        gate = dot_nn(normed_ref[...], gate_ref[...])
        up = dot_nn(normed_ref[...], up_ref[...])
        grad = dot_nt(cot_ref[...], down_ref[...])
        sig = 1.0 / (1.0 + jnp.exp(-gate))
        silu = gate * sig
        activated = (silu * up).astype(bf16)
        grad_gate = (grad * up * sig * (1.0 + gate * (1.0 - sig))).astype(bf16)
        grad_up = (grad * silu).astype(bf16)
        made = [activated, grad_gate, grad_up]
        first = pl.program_id(0) == 0

        def store(refs):
            at = 0
            for ref in refs:
                for i in range(ref.shape[0]):
                    ref[i] = made[at]
                    at += 1

        if packs == 1:
            store(out_refs)
        else:
            for pack in range(packs):
                mine = pl.program_id(0) // steps == pack
                pl.when(mine)(lambda pack=pack: store(out_refs[pack * len(parts) : (pack + 1) * len(parts)]))

        @pl.when(first)
        def _():
            down_sum[...] = dot_nn(activated, down_ref[...])
            back_sum[...] = dot_nt(grad_gate, gate_ref[...]) + dot_nt(grad_up, up_ref[...])

        @pl.when(jnp.logical_not(first))
        def _():
            down_sum[...] += dot_nn(activated, down_ref[...])
            back_sum[...] += dot_nt(grad_gate, gate_ref[...]) + dot_nt(grad_up, up_ref[...])

    held = whole((count, width))
    columns = pl.BlockSpec((width, tile), lambda i: (0, base + i))

    def piece(pack, n):
        return pl.BlockSpec(
            (n, count, tile), lambda i: (0, 0, jnp.clip(i - pack * steps, 0, steps - 1))
        )

    return call(
        body,
        (size // tile,),
        [held, held, columns, columns, pl.BlockSpec((tile, width), lambda i: (base + i, 0))],
        [piece(pack, n) for pack in range(packs) for n in parts] + [held, held],
        [shape_of((n, count, size // packs), bf16) for _ in range(packs) for n in parts]
        + [shape_of((count, width), f32)] * 2,
        12 * count * width * size,
        2 * (3 * width * size + 3 * count * size + 6 * count * width),
    )(normed, cot, gate_weight, up_weight, down_weight)


def weight_grad(buffer, total, start, lefts, chosen, rights):
    entries, count, size = rights[0].shape
    own = lefts[0][0].shape[1]
    tile = tile_of(start, size)
    base, steps = start // tile, size // tile
    sources = len(rights)
    given = 0 if buffer is None else 1

    def body(*refs):
        out_ref = refs[-1]
        rights_at = refs[given + sources * len(lefts) : -1]

        def product(which):
            left = refs[given + sources * which : given + sources * (which + 1)]
            out_ref[...] = sum(dot_tn(a[...], b[0]) for a, b in zip(left, rights_at)).astype(bf16)

        for which in range(len(lefts)):
            if len(lefts) == 1:
                product(0)
            else:
                mine = [v for v in range(entries) if chosen[v] == which]
                v = pl.program_id(0)
                pl.when((v >= mine[0]) & (v <= mine[-1]))(lambda which=which: product(which))

    return call(
        body,
        (entries, steps),
        [pl.BlockSpec(memory_space=pl.ANY)] * given
        + [whole((count, own))] * (sources * len(lefts))
        + [pl.BlockSpec((1, count, tile), lambda v, i: (v, 0, i))] * sources,
        pl.BlockSpec((own, tile), lambda v, i: (0, base + v * steps + i)),
        shape_of((own, total), bf16),
        2 * entries * sources * count * own * size,
        2 * entries * size * (sources * count + own),
        input_output_aliases={0: 0} if given else {},
    )(*([] if buffer is None else [buffer]), *(p for left in lefts for p in left), *rights)


def xor_pairs(count, bit):
    return [(i, i ^ bit) for i in range(count)]


def dp_bits():
    count = lax.axis_size("dp")
    bits = []
    bit = count // 2
    while bit:
        bits.append(bit)
        bit //= 2
    return count, bits


def moved_dp(parts, bit):
    found = []
    for part in parts:
        found.append(lax.ppermute(part, "dp", xor_pairs(lax.axis_size("dp"), bit)))
    return found


def dp_rows(rows):
    _, bits = dp_bits()
    found = [rows]
    for bit in bits:
        found = found + moved_dp(found, bit)
    return found


def halves(part, bit):
    half = part.shape[1] // 2
    upper = (lax.axis_index("dp") // bit) % 2
    keep = lax.dynamic_slice_in_dim(part, upper * half, half, 1)
    return keep, lax.dynamic_slice_in_dim(part, (1 - upper) * half, half, 1)


def dp_columns(cut):
    _, bits = dp_bits()
    for stage, bit in enumerate(bits):
        if stage:
            cut = list(zip(*(halves(part, bit) for part in found)))
        else:
            cut = [[cut[0]], [cut[1]]]
        found = list(cut[0]) + moved_dp(cut[1], bit)
    return found


def swap_tensor(values):
    return lax.ppermute(values, "tensor", [(0, 1), (1, 0)])


def sum_share(part):
    ranks = lax.axis_size("tensor")
    if ranks != 2:
        return lax.psum_scatter(part.astype(bf16), "tensor", scatter_dimension=1, tiled=True).astype(f32)
    share = part.shape[1] // 2
    me = lax.axis_index("tensor")
    mine = lax.dynamic_slice_in_dim(part, me * share, share, 1)
    theirs = lax.dynamic_slice_in_dim(part, (1 - me) * share, share, 1)
    return mine + swap_tensor(theirs.astype(bf16)).astype(f32)


def sum_whole(part):
    if lax.axis_size("tensor") != 2:
        return lax.psum(part.astype(bf16), "tensor").astype(f32)
    low = part.astype(bf16)
    return low.astype(f32) + swap_tensor(low).astype(f32)


def other_weight(weight, pieces=2):
    count, _ = dp_bits()
    size = weight.shape[0] // count // pieces
    found = []
    for at in range(pieces):
        start = (lax.axis_index("dp") * pieces + at) * size
        own = lax.dynamic_slice_in_dim(weight, start, size, 0)
        found.append(dp_rows(swap_tensor(own)))
    return found


def join_branch(base, theirs, pieces, gain):
    count, width = base.shape
    dp, bits = dp_bits()
    size = pieces[0][0].shape[0]
    parts = len(theirs)
    half = width // 2
    order = [0]
    for bit in bits:
        order = order + [at ^ bit for at in order]

    def body(base_ref, gain_ref, *refs):
        theirs_refs, piece_refs = refs[:parts], refs[parts:-5]
        hidden_ref, scale_ref, normed_ref, keep_ref, give_ref = refs[-5:]
        me = lax.axis_index("dp")
        total = base_ref[...]
        for i, ref in enumerate(piece_refs):
            piece, quarter = divmod(i, len(order))
            at = pl.multiple_of(((me ^ order[quarter]) * len(pieces) + piece) * size, size)
            left = jnp.concatenate([part[:, pl.ds(at, size)] for part in theirs_refs], axis=0)
            total = total + dot_nn(left, ref[...])
        hidden_ref[...] = total
        scale = lax.rsqrt(jnp.mean(total * total, axis=-1, keepdims=True) + norm_eps)
        scale_ref[...] = scale
        normed = (total * scale * gain_ref[...].astype(f32)).astype(bf16)
        normed_ref[...] = normed
        upper = (me // bits[0]) % 2 == 1
        keep_ref[...] = jnp.where(upper, normed[:, half:], normed[:, :half])
        give_ref[...] = jnp.where(upper, normed[:, :half], normed[:, half:])

    cut = whole((count, half))
    return call(
        body,
        (1,),
        [whole(base.shape), whole(gain.shape)]
        + [whole(p.shape) for p in theirs]
        + [whole(p.shape) for piece in pieces for p in piece],
        [whole(base.shape), whole((count, 1)), whole(base.shape), cut, cut],
        [shape_of(base.shape, f32), shape_of((count, 1), f32), shape_of(base.shape, bf16)]
        + [shape_of((count, half), bf16)] * 2,
        2 * count * width * size * len(pieces) * dp,
        2 * (6 * count * width + width * size * len(pieces) * dp),
    )(base, gain, *theirs, *(p for piece in pieces for p in piece))


def ctx_scatter(block):
    return lax.psum_scatter(block, "ctx", scatter_dimension=0, tiled=True)


def ctx_ring(block):
    count = lax.axis_size("ctx")
    me = lax.axis_index("ctx")
    size = block.shape[0] // count

    def part(back):
        at = (me - back + count) % count
        return lax.dynamic_slice_in_dim(block, at * size, size, 0)

    total = part(1)
    for step in range(count - 1):
        moved = lax.ppermute(total, "ctx", [(i, (i + 1) % count) for i in range(count)])
        total = (moved.astype(f32) + part(step + 2).astype(f32)).astype(bf16)
    return total


def gains_own(parts):
    if lax.axis_size("tensor") == 2:
        parts = parts + swap_tensor(parts)
    else:
        parts = lax.psum(parts, "tensor")
    count, bits = dp_bits()
    me = lax.axis_index("dp")
    for bit in bits:
        half = parts.shape[1] // 2
        upper = (me // bit) % 2
        keep = lax.dynamic_slice_in_dim(parts, upper * half, half, 1)
        give = lax.dynamic_slice_in_dim(parts, (1 - upper) * half, half, 1)
        parts = keep + lax.ppermute(give, "dp", xor_pairs(count, bit))
    return parts


def shards(
    block_in,
    attn_gain,
    query_weight,
    key_weight,
    value_weight,
    output_weight,
    mlp_gain,
    gate_weight,
    up_weight,
    down_weight,
    cotangent,
):
    seq_count, ctx_tok, width = block_in.shape
    ctx_ranks = lax.axis_size("ctx")
    tensor_ranks = lax.axis_size("tensor")
    share_len = ctx_tok // tensor_ranks
    share_start = lax.axis_index("tensor") * share_len
    rows = seq_count * ctx_tok
    query_cols = query_weight.shape[1]
    kv_cols = key_weight.shape[1]
    units = gate_weight.shape[1]
    ctx_at = lax.axis_index("ctx")
    deep = (seq_count, ctx_tok, width)

    def share_of(values):
        return lax.dynamic_slice_in_dim(values, share_start, share_len, 1)

    gain_first = attn_gain.astype(f32)
    gain_second = mlp_gain.astype(f32)
    flat_in = block_in.reshape(rows, width)
    cot_rows = cotangent.reshape(rows, width)
    positions = ctx_at * ctx_tok + jnp.arange(ctx_tok, dtype=jnp.int32)
    cosine, sine = rope_columns(positions)
    ones = jnp.ones((ctx_tok, kv_cols), f32)
    table = lambda one, rest: jnp.concatenate(
        [jnp.tile(one[:, :HD], (1, kv_cols // HD)), rest], axis=1
    )
    kv_cosine, kv_sine = table(cosine, ones), table(sine, ones * 0.0)

    normed, kv_own = norm_kv(
        flat_in, attn_gain[None], key_weight, value_weight, kv_cosine, kv_sine
    )
    kv_blocks = [kv_own]
    for back in range(1, ctx_ranks):
        kv_blocks.append(
            lax.ppermute(kv_own, "ctx", [(i, i + back) for i in range(ctx_ranks - back)])
        )
    queries = project_queries(normed, query_weight, cosine, sine)
    parts = []
    for seq in range(seq_count):
        parts.append(attend(queries, kv_blocks, ctx_tok, seq))
    attended = jnp.concatenate(parts, axis=0)
    branch = dot_nn(attended, output_weight)
    if tensor_ranks == 2:
        theirs = [swap_tensor(part) for part in parts]
        pieces = other_weight(output_weight)
        hidden, r_second, normed_mlp, *nm_cut = join_branch(
            flat_in.astype(f32) + branch, theirs, pieces, mlp_gain[None]
        )
    else:
        hidden = flat_in.astype(f32) + lax.psum(branch, "tensor")
        r_second = lax.rsqrt(jnp.mean(hidden * hidden, axis=-1, keepdims=True) + norm_eps)
        normed_mlp = (hidden * r_second * gain_second).astype(bf16)
        nm_cut = halves(normed_mlp, dp_bits()[1][0])

    unit = units // 4
    weights = (gate_weight, up_weight, down_weight)
    act_0, grads_0, down_0, back_0 = mlp(normed_mlp, cot_rows, *weights, 0, unit, (1, 2))
    pack_1, down_1, back_1 = mlp(normed_mlp, cot_rows, *weights, unit, unit, (3,))
    pack_2, pack_3, down_2, back_2 = mlp(
        normed_mlp, cot_rows, *weights, 2 * unit, 2 * unit, (3,), 2
    )
    mlp_part = down_0 + down_1 + down_2
    back_part = back_0 + back_1 + back_2

    cot_cols = dp_columns(halves(cot_rows, dp_bits()[1][0]))
    normed_cols = dp_columns(halves(normed, dp_bits()[1][0]))
    attended_all = dp_rows(attended[None])
    nm_cols = dp_columns(nm_cut)
    both = [cot_cols, nm_cols]
    act_0 = dp_rows(act_0)
    grads_0 = dp_rows(grads_0)
    pack_1, pack_2 = dp_rows(pack_1), dp_rows(pack_2)
    pack_3 = dp_rows(pack_3)
    wg_0 = weight_grad(None, unit, 0, [cot_cols], (0,), act_0)
    wg_1 = weight_grad(None, 2 * unit, 0, [nm_cols], (0, 0), grads_0)
    wg_2 = weight_grad(None, 3 * unit, 0, both, (0, 1, 1), pack_1)
    wg_3 = weight_grad(None, 3 * unit, 0, both, (0, 1, 1), pack_2)
    wg_4 = weight_grad(None, 3 * unit, 0, both, (0, 1, 1), pack_3)
    first_sum = ctx_scatter(wg_0)
    second_sum = ctx_scatter(wg_1)
    third_sum = ctx_scatter(wg_2)
    ring_sum = ctx_ring(wg_3)
    fourth_sum = ctx_scatter(wg_4)
    qkv_cols = query_cols + 2 * kv_cols
    total = qkv_cols + query_cols + 128

    hidden_deep = hidden.reshape(deep)
    block_out = (share_of(hidden_deep) + sum_share(mlp_part.reshape(deep))).astype(bf16)
    unit_second = hidden * r_second
    mlp_gain_part = jnp.sum(back_part * unit_second, axis=0)
    scaled = gain_second * sum_whole(back_part)
    grad_hidden = cot_rows.astype(f32) + r_second * (
        scaled - unit_second * jnp.mean(scaled * unit_second, axis=-1, keepdims=True)
    )
    grad_branch = grad_hidden.astype(bf16)
    grad_attended = dot_nt(grad_branch, output_weight).astype(bf16)
    branch_cols = dp_columns(halves(grad_branch, dp_bits()[1][0]))
    last = weight_grad(None, total, qkv_cols, [branch_cols], (0,), attended_all)

    grad_query_raw, kv_sum, *kv_given = attend_back(
        queries, kv_blocks, grad_attended, cosine, sine, ctx_tok
    )
    for back, piece in enumerate(kv_given, 1):
        given = lax.ppermute(piece, "ctx", [(i + back, i) for i in range(ctx_ranks - back)])
        kv_sum = kv_sum + given.astype(f32)
    kv_sum = kv_sum.reshape(seq_count, ctx_tok, 2, kv_cols // HD, 2, HD // 2)
    first_half, second_half = kv_sum[..., 0, :], kv_sum[..., 1, :]
    cos_half = jnp.stack([cosine[:, : HD // 2], ones[:, : HD // 2]], axis=1)[:, :, None]
    sin_half = jnp.stack([sine[:, HD // 2 : HD], ones[:, : HD // 2] * 0.0], axis=1)[:, :, None]
    grad_kv_raw = (
        jnp.stack(
            [
                first_half * cos_half + second_half * sin_half,
                second_half * cos_half - first_half * sin_half,
            ],
            axis=-2,
        )
        .astype(bf16)
        .reshape(rows, 2 * kv_cols)
    )
    grad_raw = jnp.concatenate([grad_query_raw, grad_kv_raw], axis=1)
    raw_all = dp_rows(grad_raw[None])
    last = weight_grad(last, total, 0, [normed_cols], (0,), raw_all)
    grad_normed_first = (
        dot_nt(grad_query_raw, query_weight)
        + dot_nt(grad_kv_raw[:, :kv_cols], key_weight)
        + dot_nt(grad_kv_raw[:, kv_cols:], value_weight)
    )
    full_in = flat_in.astype(f32)
    r_first = lax.rsqrt(jnp.mean(full_in * full_in, axis=-1, keepdims=True) + norm_eps)
    unit_first = full_in * r_first
    attn_gain_part = jnp.sum(grad_normed_first * unit_first, axis=0)
    gains = gains_own(jnp.stack([attn_gain_part, mlp_gain_part]))
    gain_block = jnp.pad(gains.T.astype(bf16), ((0, 0), (0, 126)))
    last = lax.dynamic_update_slice(last, gain_block, (0, total - 128))
    last_sum = ctx_scatter(last)

    scaled_first = gain_first * sum_share(grad_normed_first.reshape(deep))
    unit_share = share_of(unit_first.reshape(deep))
    input_grad = share_of(grad_hidden.reshape(deep)) + share_of(r_first.reshape(seq_count, ctx_tok, 1)) * (
        scaled_first - unit_share * jnp.mean(scaled_first * unit_share, axis=-1, keepdims=True)
    )

    def joined(*parts):
        return jnp.concatenate(parts, axis=1).astype(f32)

    piece = lambda summed, at: summed[:, at * unit : (at + 1) * unit]
    grad_down = joined(first_sum, piece(third_sum, 0), piece(ring_sum, 0), piece(fourth_sum, 0)).T
    grad_gate = joined(
        piece(second_sum, 0), piece(third_sum, 1), piece(ring_sum, 1), piece(fourth_sum, 1)
    )
    grad_up = joined(
        piece(second_sum, 1), piece(third_sum, 2), piece(ring_sum, 2), piece(fourth_sum, 2)
    )
    query_end = query_cols
    key_end = query_end + kv_cols
    value_end = key_end + kv_cols
    cut = lambda first, end: last_sum[:, first:end].astype(f32)
    gains_out = cut(total - 128, total - 126)
    return (
        block_out,
        input_grad,
        gains_out[:, 0],
        cut(0, query_end),
        cut(query_end, key_end),
        cut(key_end, value_end),
        cut(value_end, total - 128).T,
        gains_out[:, 1],
        grad_gate,
        grad_up,
        grad_down,
    )


def solution(mesh):
    in_specs = (
        P("dp", "ctx", None),
        P(),
        P(None, "tensor"),
        P(None, "tensor"),
        P(None, "tensor"),
        P("tensor", None),
        P(),
        P(None, "tensor"),
        P(None, "tensor"),
        P("tensor", None),
        P("dp", "ctx", None),
    )
    out_specs = (
        P("dp", ("ctx", "tensor"), None),
        P("dp", ("ctx", "tensor"), None),
        P(("dp", "ctx")),
        P(("dp", "ctx"), "tensor"),
        P(("dp", "ctx"), "tensor"),
        P(("dp", "ctx"), "tensor"),
        P("tensor", ("dp", "ctx")),
        P(("dp", "ctx")),
        P(("dp", "ctx"), "tensor"),
        P(("dp", "ctx"), "tensor"),
        P("tensor", ("dp", "ctx")),
    )

    return jax.shard_map(shards, mesh=mesh, in_specs=in_specs, out_specs=out_specs, check_vma=False)
```

```python
import jax
import jax.numpy as jnp
from jax import lax
from jax.experimental import pallas as pl
from jax.experimental.pallas import tpu as pltpu
from jax.sharding import PartitionSpec as P


HD = 64

norm_eps = 1e-05
rope_base = 500000.0
f32 = jnp.float32
bf16 = jnp.bfloat16


def rms_apply(values, gain):
    return values * lax.rsqrt(jnp.mean(values * values, axis=-1, keepdims=True) + norm_eps) * gain


def rope_tables(positions, head_size):
    half_width = head_size // 2
    frequency = rope_base ** (-jnp.arange(half_width, dtype=f32) * 2.0 / head_size)
    angles = positions.astype(f32)[:, None] * frequency[None, :]
    return (jnp.cos(angles)[:, None, :], jnp.sin(angles)[:, None, :])


def dot_nn(left, right):
    return lax.dot_general(left, right, (((1,), (0,)), ((), ())), preferred_element_type=f32)


def dot_tn(left, right):
    return lax.dot_general(left, right, (((0,), (0,)), ((), ())), preferred_element_type=f32)


def dot_nt(left, right):
    return lax.dot_general(left, right, (((1,), (1,)), ((), ())), preferred_element_type=f32)


def call(body, grid, in_specs, out_specs, out_shape, flops, moved, **rest):
    return pl.pallas_call(
        body,
        grid=grid,
        in_specs=in_specs,
        out_specs=out_specs,
        out_shape=out_shape,
        cost_estimate=pl.CostEstimate(flops=flops, bytes_accessed=moved, transcendentals=0),
        compiler_params=pltpu.CompilerParams(vmem_limit_bytes=56 << 20),
        **rest,
    )


def whole(shape):
    zeros = (0,) * len(shape)
    return pl.BlockSpec(shape, lambda *_: zeros, pipeline_mode=pl.Buffered(1))


def shape_of(shape, kind):
    return jax.ShapeDtypeStruct(shape, kind)


def turned(values, cosine, sine):
    at = lax.broadcasted_iota(jnp.int32, values.shape, 1) % HD
    swapped = jnp.where(
        at < HD // 2, pltpu.roll(values, 128 - HD // 2, 1), pltpu.roll(values, HD // 2, 1)
    )
    return values * cosine + swapped * sine


def rope_columns(positions):
    cosine, sine = rope_tables(positions, HD)
    cosine, sine = cosine[:, 0], sine[:, 0]
    return jnp.tile(cosine, (1, 4)), jnp.tile(jnp.concatenate([-sine, sine], axis=-1), (1, 2))


def norm_kv(rows, gain, key_weight, value_weight, cosine, sine):
    count, width = rows.shape
    cols = key_weight.shape[1]
    tokens = cosine.shape[0]

    def body(rows_ref, gain_ref, key_ref, value_ref, cos_ref, sin_ref, normed_ref, kv_ref):
        values = rows_ref[...].astype(f32)
        normed = rms_apply(values, gain_ref[...].astype(f32)).astype(bf16)
        normed_ref[...] = normed
        raw = jnp.concatenate([dot_nn(normed, key_ref[...]), dot_nn(normed, value_ref[...])], axis=1)
        for first in range(0, count, tokens):
            for at in range(0, 2 * cols, 128):
                part = raw[first : first + tokens, at : at + 128]
                kv_ref[first : first + tokens, at : at + 128] = turned(
                    part, cos_ref[:, at : at + 128], sin_ref[:, at : at + 128]
                ).astype(bf16)

    shapes = [rows.shape, gain.shape, key_weight.shape, value_weight.shape, cosine.shape, sine.shape]
    return call(
        body,
        (1,),
        [whole(s) for s in shapes],
        [whole(rows.shape), whole((count, 2 * cols))],
        [shape_of(rows.shape, bf16), shape_of((count, 2 * cols), bf16)],
        4 * count * width * cols,
        2 * (2 * count * width + 2 * width * cols),
    )(rows, gain, key_weight, value_weight, cosine, sine)


def tile_of(*sizes):
    for tile in (512, 256, 128):
        if all(size % tile == 0 for size in sizes):
            return tile
    raise ValueError("no tile")


def project_queries(normed, weight, cosine, sine):
    count, width = normed.shape
    cols = weight.shape[1]
    tokens = cosine.shape[0]
    tile = tile_of(cols)

    def body(normed_ref, weight_ref, cos_ref, sin_ref, out_ref):
        raw = dot_nn(normed_ref[...], weight_ref[...])
        for first in range(0, count, tokens):
            for at in range(0, tile, 128):
                out_ref[first : first + tokens, at : at + 128] = turned(
                    raw[first : first + tokens, at : at + 128], cos_ref[...], sin_ref[...]
                ).astype(bf16)

    return call(
        body,
        (cols // tile,),
        [
            whole(normed.shape),
            pl.BlockSpec((width, tile), lambda i: (0, i)),
            whole(cosine.shape),
            whole(sine.shape),
        ],
        pl.BlockSpec((count, tile), lambda i: (0, i)),
        shape_of((count, cols), bf16),
        2 * count * width * cols,
        2 * (count * width + width * cols),
    )(normed, weight, cosine, sine)


def probs_of(stacked, keys, tokens, ctx_at, scale):
    raw = dot_nt(stacked, keys) * scale
    found = []
    for back in range(keys.shape[0] // tokens):
        part = raw[:, back * tokens : (back + 1) * tokens]
        if back == 0:
            query_at = lax.broadcasted_iota(jnp.int32, part.shape, 0) % tokens
            seen = query_at >= lax.broadcasted_iota(jnp.int32, part.shape, 1)
            found.append(jnp.where(seen, part, -1e30))
        else:
            found.append(part + jnp.where(ctx_at >= back, 0.0, -1e30).astype(f32))
    most = found[0]
    for part in found[1:]:
        most = jnp.maximum(most, part)
    most = jnp.max(most, axis=-1, keepdims=True)
    found = [jnp.exp(part - most) for part in found]
    inverse = 1.0 / jnp.sum(sum(found), axis=-1, keepdims=True)
    return jnp.concatenate([part * inverse for part in found], axis=1)


def stack_heads(ref, head, group):
    first = head * group
    return jnp.concatenate(
        [ref[:, (first + g) * HD : (first + g + 1) * HD] for g in range(group)], axis=0
    )


def attend(queries, kv_blocks, tokens, seq):
    _, cols = queries.shape
    kv_cols = kv_blocks[0].shape[1] // 2
    heads = kv_cols // HD
    group = cols // kv_cols
    scale = HD ** (-0.5)
    blocks = len(kv_blocks)

    def body(query_ref, *refs):
        out_ref = refs[-1]
        ctx_at = lax.axis_index("ctx")
        for head in range(heads):
            stacked = stack_heads(query_ref, head, group)
            at = head * HD
            keys = jnp.concatenate([ref[:, at : at + HD] for ref in refs[:blocks]], axis=0)
            at += kv_cols
            values = jnp.concatenate([ref[:, at : at + HD] for ref in refs[:blocks]], axis=0)
            probs = probs_of(stacked, keys, tokens, ctx_at, scale)
            total = dot_nn(probs.astype(bf16), values)
            for g in range(group):
                first = (head * group + g) * HD
                out_ref[:, first : first + HD] = total[g * tokens : (g + 1) * tokens].astype(bf16)

    rows = lambda width: pl.BlockSpec((tokens, width), lambda i: (seq, 0))
    return call(
        body,
        (1,),
        [rows(cols)] + [rows(2 * kv_cols)] * blocks,
        whole((tokens, cols)),
        shape_of((tokens, cols), bf16),
        40 * tokens * cols * tokens * blocks,
        2 * tokens * (2 * cols + 2 * kv_cols * blocks),
    )(queries, *kv_blocks)


def attend_back(queries, kv_blocks, grad_attended, cosine, sine, tokens):
    count, cols = queries.shape
    kv_cols = kv_blocks[0].shape[1] // 2
    heads = kv_cols // HD
    group = cols // kv_cols
    scale = HD ** (-0.5)
    blocks = len(kv_blocks)

    def body(query_ref, grad_ref, cos_ref, sin_ref, *refs):
        kv_refs, query_out, kv_out = refs[:blocks], refs[blocks], refs[blocks + 1 : -1]
        turned_ref = refs[-1]
        ctx_at = lax.axis_index("ctx")
        for head in range(heads):
            stacked = stack_heads(query_ref, head, group)
            grads = stack_heads(grad_ref, head, group)
            at = head * HD
            keys = jnp.concatenate([ref[:, at : at + HD] for ref in kv_refs], axis=0)
            end = kv_cols + at
            values = jnp.concatenate([ref[:, end : end + HD] for ref in kv_refs], axis=0)
            probs = probs_of(stacked, keys, tokens, ctx_at, scale)
            grad_probs = dot_nt(grads, values)
            inner = jnp.sum(probs * grad_probs, axis=-1, keepdims=True)
            grad_scores = (probs * (grad_probs - inner)).astype(bf16)
            total = dot_nn(grad_scores, keys)
            grad_keys = dot_tn(grad_scores, stacked) * scale
            grad_values = dot_tn(probs.astype(bf16), grads)
            for back, ref in enumerate(kv_out):
                mine = slice(back * tokens, (back + 1) * tokens)
                ref[:, at : at + HD] = grad_keys[mine].astype(ref.dtype)
                ref[:, end : end + HD] = grad_values[mine].astype(ref.dtype)
            for g in range(group):
                first = (head * group + g) * HD
                turned_ref[:, first : first + HD] = total[g * tokens : (g + 1) * tokens] * scale
        for at in range(0, cols, 128):
            query_out[:, at : at + 128] = turned(
                turned_ref[:, at : at + 128], cos_ref[...], -sin_ref[...]
            ).astype(bf16)

    rows = lambda width: pl.BlockSpec((tokens, width), lambda i: (i, 0))
    return call(
        body,
        (count // tokens,),
        [rows(cols), rows(cols), whole(cosine.shape), whole(sine.shape)]
        + [rows(2 * kv_cols)] * blocks,
        [rows(cols)] + [rows(2 * kv_cols)] * blocks,
        [shape_of((count, cols), bf16)]
        + [shape_of((count, 2 * kv_cols), f32 if back == 0 else bf16) for back in range(blocks)],
        100 * count * cols * tokens * blocks,
        2 * count * (3 * cols + 4 * kv_cols * blocks),
        scratch_shapes=[pltpu.VMEM((tokens, cols), f32)],
    )(queries, grad_attended, cosine, sine, *kv_blocks)


def mlp(normed, cot, gate_weight, up_weight, down_weight, start, size, parts, packs=1):
    count, width = normed.shape
    tile = tile_of(start, size // packs)
    base = start // tile
    steps = size // packs // tile

    def body(normed_ref, cot_ref, gate_ref, up_ref, down_ref, *refs):
        out_refs, down_sum, back_sum = refs[:-2], refs[-2], refs[-1]
        gate = dot_nn(normed_ref[...], gate_ref[...])
        up = dot_nn(normed_ref[...], up_ref[...])
        grad = dot_nt(cot_ref[...], down_ref[...])
        sig = 1.0 / (1.0 + jnp.exp(-gate))
        silu = gate * sig
        activated = (silu * up).astype(bf16)
        grad_gate = (grad * up * sig * (1.0 + gate * (1.0 - sig))).astype(bf16)
        grad_up = (grad * silu).astype(bf16)
        made = [activated, grad_gate, grad_up]
        first = pl.program_id(0) == 0

        def store(refs):
            at = 0
            for ref in refs:
                for i in range(ref.shape[0]):
                    ref[i] = made[at]
                    at += 1

        if packs == 1:
            store(out_refs)
        else:
            for pack in range(packs):
                mine = pl.program_id(0) // steps == pack
                pl.when(mine)(lambda pack=pack: store(out_refs[pack * len(parts) : (pack + 1) * len(parts)]))

        @pl.when(first)
        def _():
            down_sum[...] = dot_nn(activated, down_ref[...])
            back_sum[...] = dot_nt(grad_gate, gate_ref[...]) + dot_nt(grad_up, up_ref[...])

        @pl.when(jnp.logical_not(first))
        def _():
            down_sum[...] += dot_nn(activated, down_ref[...])
            back_sum[...] += dot_nt(grad_gate, gate_ref[...]) + dot_nt(grad_up, up_ref[...])

    held = whole((count, width))
    columns = pl.BlockSpec((width, tile), lambda i: (0, base + i))

    def piece(pack, n):
        return pl.BlockSpec(
            (n, count, tile), lambda i: (0, 0, jnp.clip(i - pack * steps, 0, steps - 1))
        )

    return call(
        body,
        (size // tile,),
        [held, held, columns, columns, pl.BlockSpec((tile, width), lambda i: (base + i, 0))],
        [piece(pack, n) for pack in range(packs) for n in parts] + [held, held],
        [shape_of((n, count, size // packs), bf16) for _ in range(packs) for n in parts]
        + [shape_of((count, width), f32)] * 2,
        12 * count * width * size,
        2 * (3 * width * size + 3 * count * size + 6 * count * width),
    )(normed, cot, gate_weight, up_weight, down_weight)


def weight_grad(buffer, total, start, lefts, chosen, rights):
    entries, count, size = rights[0].shape
    own = lefts[0][0].shape[1]
    tile = tile_of(start, size)
    base, steps = start // tile, size // tile
    sources = len(rights)
    given = 0 if buffer is None else 1

    def body(*refs):
        out_ref = refs[-1]
        rights_at = refs[given + sources * len(lefts) : -1]

        def product(which):
            left = refs[given + sources * which : given + sources * (which + 1)]
            out_ref[...] = sum(dot_tn(a[...], b[0]) for a, b in zip(left, rights_at)).astype(bf16)

        for which in range(len(lefts)):
            if len(lefts) == 1:
                product(0)
            else:
                mine = [v for v in range(entries) if chosen[v] == which]
                v = pl.program_id(0)
                pl.when((v >= mine[0]) & (v <= mine[-1]))(lambda which=which: product(which))

    return call(
        body,
        (entries, steps),
        [pl.BlockSpec(memory_space=pl.ANY)] * given
        + [whole((count, own))] * (sources * len(lefts))
        + [pl.BlockSpec((1, count, tile), lambda v, i: (v, 0, i))] * sources,
        pl.BlockSpec((own, tile), lambda v, i: (0, base + v * steps + i)),
        shape_of((own, total), bf16),
        2 * entries * sources * count * own * size,
        2 * entries * size * (sources * count + own),
        input_output_aliases={0: 0} if given else {},
    )(*([] if buffer is None else [buffer]), *(p for left in lefts for p in left), *rights)


def xor_pairs(count, bit):
    return [(i, i ^ bit) for i in range(count)]


def dp_bits():
    count = lax.axis_size("dp")
    bits = []
    bit = count // 2
    while bit:
        bits.append(bit)
        bit //= 2
    return count, bits


def moved_dp(parts, bit):
    found = []
    for part in parts:
        found.append(lax.ppermute(part, "dp", xor_pairs(lax.axis_size("dp"), bit)))
    return found


def dp_rows(rows):
    _, bits = dp_bits()
    found = [rows]
    for bit in bits:
        found = found + moved_dp(found, bit)
    return found


def halves(part, bit):
    half = part.shape[1] // 2
    upper = (lax.axis_index("dp") // bit) % 2
    keep = lax.dynamic_slice_in_dim(part, upper * half, half, 1)
    return keep, lax.dynamic_slice_in_dim(part, (1 - upper) * half, half, 1)


def dp_columns(cut):
    _, bits = dp_bits()
    for stage, bit in enumerate(bits):
        if stage:
            cut = list(zip(*(halves(part, bit) for part in found)))
        else:
            cut = [[cut[0]], [cut[1]]]
        found = list(cut[0]) + moved_dp(cut[1], bit)
    return found


def swap_tensor(values):
    return lax.ppermute(values, "tensor", [(0, 1), (1, 0)])


def sum_share(part):
    ranks = lax.axis_size("tensor")
    if ranks != 2:
        return lax.psum_scatter(part.astype(bf16), "tensor", scatter_dimension=1, tiled=True).astype(f32)
    share = part.shape[1] // 2
    me = lax.axis_index("tensor")
    mine = lax.dynamic_slice_in_dim(part, me * share, share, 1)
    theirs = lax.dynamic_slice_in_dim(part, (1 - me) * share, share, 1)
    return mine + swap_tensor(theirs.astype(bf16)).astype(f32)


def sum_whole(part):
    if lax.axis_size("tensor") != 2:
        return lax.psum(part.astype(bf16), "tensor").astype(f32)
    low = part.astype(bf16)
    return low.astype(f32) + swap_tensor(low).astype(f32)


def other_weight(weight, pieces=2):
    count, _ = dp_bits()
    size = weight.shape[0] // count // pieces
    found = []
    for at in range(pieces):
        start = (lax.axis_index("dp") * pieces + at) * size
        own = lax.dynamic_slice_in_dim(weight, start, size, 0)
        found.append(dp_rows(swap_tensor(own)))
    return found


def join_branch(base, theirs, pieces, gain):
    count, width = base.shape
    dp, bits = dp_bits()
    size = pieces[0][0].shape[0]
    parts = len(theirs)
    half = width // 2
    order = [0]
    for bit in bits:
        order = order + [at ^ bit for at in order]

    def body(base_ref, gain_ref, *refs):
        theirs_refs, piece_refs = refs[:parts], refs[parts:-5]
        hidden_ref, scale_ref, normed_ref, keep_ref, give_ref = refs[-5:]
        me = lax.axis_index("dp")
        total = base_ref[...]
        for i, ref in enumerate(piece_refs):
            piece, quarter = divmod(i, len(order))
            at = pl.multiple_of(((me ^ order[quarter]) * len(pieces) + piece) * size, size)
            left = jnp.concatenate([part[:, pl.ds(at, size)] for part in theirs_refs], axis=0)
            total = total + dot_nn(left, ref[...])
        hidden_ref[...] = total
        scale = lax.rsqrt(jnp.mean(total * total, axis=-1, keepdims=True) + norm_eps)
        scale_ref[...] = scale
        normed = (total * scale * gain_ref[...].astype(f32)).astype(bf16)
        normed_ref[...] = normed
        upper = (me // bits[0]) % 2 == 1
        keep_ref[...] = jnp.where(upper, normed[:, half:], normed[:, :half])
        give_ref[...] = jnp.where(upper, normed[:, :half], normed[:, half:])

    cut = whole((count, half))
    return call(
        body,
        (1,),
        [whole(base.shape), whole(gain.shape)]
        + [whole(p.shape) for p in theirs]
        + [whole(p.shape) for piece in pieces for p in piece],
        [whole(base.shape), whole((count, 1)), whole(base.shape), cut, cut],
        [shape_of(base.shape, f32), shape_of((count, 1), f32), shape_of(base.shape, bf16)]
        + [shape_of((count, half), bf16)] * 2,
        2 * count * width * size * len(pieces) * dp,
        2 * (6 * count * width + width * size * len(pieces) * dp),
    )(base, gain, *theirs, *(p for piece in pieces for p in piece))


def ctx_scatter(block):
    return lax.psum_scatter(block, "ctx", scatter_dimension=0, tiled=True)


def ctx_ring(block):
    count = lax.axis_size("ctx")
    me = lax.axis_index("ctx")
    size = block.shape[0] // count

    def part(back):
        at = (me - back + count) % count
        return lax.dynamic_slice_in_dim(block, at * size, size, 0)

    total = part(1)
    for step in range(count - 1):
        moved = lax.ppermute(total, "ctx", [(i, (i + 1) % count) for i in range(count)])
        total = (moved.astype(f32) + part(step + 2).astype(f32)).astype(bf16)
    return total


def gains_own(parts):
    if lax.axis_size("tensor") == 2:
        parts = parts + swap_tensor(parts)
    else:
        parts = lax.psum(parts, "tensor")
    count, bits = dp_bits()
    me = lax.axis_index("dp")
    for bit in bits:
        half = parts.shape[1] // 2
        upper = (me // bit) % 2
        keep = lax.dynamic_slice_in_dim(parts, upper * half, half, 1)
        give = lax.dynamic_slice_in_dim(parts, (1 - upper) * half, half, 1)
        parts = keep + lax.ppermute(give, "dp", xor_pairs(count, bit))
    return parts


def shards(
    block_in,
    attn_gain,
    query_weight,
    key_weight,
    value_weight,
    output_weight,
    mlp_gain,
    gate_weight,
    up_weight,
    down_weight,
    cotangent,
):
    seq_count, ctx_tok, width = block_in.shape
    ctx_ranks = lax.axis_size("ctx")
    tensor_ranks = lax.axis_size("tensor")
    share_len = ctx_tok // tensor_ranks
    share_start = lax.axis_index("tensor") * share_len
    rows = seq_count * ctx_tok
    query_cols = query_weight.shape[1]
    kv_cols = key_weight.shape[1]
    units = gate_weight.shape[1]
    ctx_at = lax.axis_index("ctx")
    deep = (seq_count, ctx_tok, width)

    def share_of(values):
        return lax.dynamic_slice_in_dim(values, share_start, share_len, 1)

    gain_first = attn_gain.astype(f32)
    gain_second = mlp_gain.astype(f32)
    flat_in = block_in.reshape(rows, width)
    cot_rows = cotangent.reshape(rows, width)
    positions = ctx_at * ctx_tok + jnp.arange(ctx_tok, dtype=jnp.int32)
    cosine, sine = rope_columns(positions)
    ones = jnp.ones((ctx_tok, kv_cols), f32)
    table = lambda one, rest: jnp.concatenate(
        [jnp.tile(one[:, :HD], (1, kv_cols // HD)), rest], axis=1
    )
    kv_cosine, kv_sine = table(cosine, ones), table(sine, ones * 0.0)

    normed, kv_own = norm_kv(flat_in, attn_gain[None], key_weight, value_weight, kv_cosine, kv_sine)
    kv_blocks = [kv_own]
    for back in range(1, ctx_ranks):
        kv_blocks.append(
            lax.ppermute(kv_own, "ctx", [(i, i + back) for i in range(ctx_ranks - back)])
        )
    queries = project_queries(normed, query_weight, cosine, sine)
    parts = []
    for seq in range(seq_count):
        parts.append(attend(queries, kv_blocks, ctx_tok, seq))
    attended = jnp.concatenate(parts, axis=0)
    branch = dot_nn(attended, output_weight)
    if tensor_ranks == 2:
        theirs = [swap_tensor(part) for part in parts]
        pieces = other_weight(output_weight)
        hidden, r_second, normed_mlp, *nm_cut = join_branch(
            flat_in.astype(f32) + branch, theirs, pieces, mlp_gain[None]
        )
    else:
        hidden = flat_in.astype(f32) + lax.psum(branch, "tensor")
        r_second = lax.rsqrt(jnp.mean(hidden * hidden, axis=-1, keepdims=True) + norm_eps)
        normed_mlp = (hidden * r_second * gain_second).astype(bf16)
        nm_cut = halves(normed_mlp, dp_bits()[1][0])

    unit = units // 4
    weights = (gate_weight, up_weight, down_weight)
    act_0, grads_0, down_0, back_0 = mlp(normed_mlp, cot_rows, *weights, 0, unit, (1, 2))
    pack_1, down_1, back_1 = mlp(normed_mlp, cot_rows, *weights, unit, unit, (3,))
    pack_2, down_2, back_2 = mlp(normed_mlp, cot_rows, *weights, 2 * unit, unit, (3,))
    pack_3, down_3, back_3 = mlp(normed_mlp, cot_rows, *weights, 3 * unit, unit, (3,))
    mlp_part = down_0 + down_1 + down_2 + down_3
    back_part = back_0 + back_1 + back_2 + back_3

    cot_cols = dp_columns(halves(cot_rows, dp_bits()[1][0]))
    normed_cols = dp_columns(halves(normed, dp_bits()[1][0]))
    attended_all = dp_rows(attended[None])
    nm_cols = dp_columns(nm_cut)
    both = [cot_cols, nm_cols]
    act_0 = dp_rows(act_0)
    grads_0 = dp_rows(grads_0)
    pack_1, pack_2 = dp_rows(pack_1), dp_rows(pack_2)
    pack_3 = dp_rows(pack_3)
    wg_0 = weight_grad(None, unit, 0, [cot_cols], (0,), act_0)
    wg_1 = weight_grad(None, 2 * unit, 0, [nm_cols], (0, 0), grads_0)
    wg_2 = weight_grad(None, 3 * unit, 0, both, (0, 1, 1), pack_1)
    wg_3 = weight_grad(None, 3 * unit, 0, both, (0, 1, 1), pack_2)
    wg_4 = weight_grad(None, 3 * unit, 0, both, (0, 1, 1), pack_3)
    first_sum = ctx_scatter(wg_0)
    second_sum = ctx_scatter(wg_1)
    third_sum = ctx_scatter(wg_2)
    ring_sum = ctx_ring(wg_3)
    fourth_sum = ctx_scatter(wg_4)
    qkv_cols = query_cols + 2 * kv_cols
    total = qkv_cols + query_cols + 128

    hidden_deep = hidden.reshape(deep)
    block_out = (share_of(hidden_deep) + sum_share(mlp_part.reshape(deep))).astype(bf16)
    unit_second = hidden * r_second
    mlp_gain_part = jnp.sum(back_part * unit_second, axis=0)
    scaled = gain_second * sum_whole(back_part)
    grad_hidden = cot_rows.astype(f32) + r_second * (
        scaled - unit_second * jnp.mean(scaled * unit_second, axis=-1, keepdims=True)
    )
    grad_branch = grad_hidden.astype(bf16)
    grad_attended = dot_nt(grad_branch, output_weight).astype(bf16)
    branch_cols = dp_columns(halves(grad_branch, dp_bits()[1][0]))
    last = weight_grad(None, total, qkv_cols, [branch_cols], (0,), attended_all)

    grad_query_raw, kv_sum, *kv_given = attend_back(
        queries, kv_blocks, grad_attended, cosine, sine, ctx_tok
    )
    for back, piece in enumerate(kv_given, 1):
        given = lax.ppermute(piece, "ctx", [(i + back, i) for i in range(ctx_ranks - back)])
        kv_sum = kv_sum + given.astype(f32)
    kv_sum = kv_sum.reshape(seq_count, ctx_tok, 2, kv_cols // HD, 2, HD // 2)
    first_half, second_half = kv_sum[..., 0, :], kv_sum[..., 1, :]
    cos_half = jnp.stack([cosine[:, : HD // 2], ones[:, : HD // 2]], axis=1)[:, :, None]
    sin_half = jnp.stack([sine[:, HD // 2 : HD], ones[:, : HD // 2] * 0.0], axis=1)[:, :, None]
    grad_kv_raw = (
        jnp.stack(
            [
                first_half * cos_half + second_half * sin_half,
                second_half * cos_half - first_half * sin_half,
            ],
            axis=-2,
        )
        .astype(bf16)
        .reshape(rows, 2 * kv_cols)
    )
    grad_raw = jnp.concatenate([grad_query_raw, grad_kv_raw], axis=1)
    raw_all = dp_rows(grad_raw[None])
    last = weight_grad(last, total, 0, [normed_cols], (0,), raw_all)
    grad_normed_first = (
        dot_nt(grad_query_raw, query_weight)
        + dot_nt(grad_kv_raw[:, :kv_cols], key_weight)
        + dot_nt(grad_kv_raw[:, kv_cols:], value_weight)
    )
    full_in = flat_in.astype(f32)
    r_first = lax.rsqrt(jnp.mean(full_in * full_in, axis=-1, keepdims=True) + norm_eps)
    unit_first = full_in * r_first
    attn_gain_part = jnp.sum(grad_normed_first * unit_first, axis=0)
    gains = gains_own(jnp.stack([attn_gain_part, mlp_gain_part]))
    gain_block = jnp.pad(gains.T.astype(bf16), ((0, 0), (0, 126)))
    last = lax.dynamic_update_slice(last, gain_block, (0, total - 128))
    last_sum = ctx_scatter(last)

    scaled_first = gain_first * sum_share(grad_normed_first.reshape(deep))
    unit_share = share_of(unit_first.reshape(deep))
    input_grad = share_of(grad_hidden.reshape(deep)) + share_of(r_first.reshape(seq_count, ctx_tok, 1)) * (
        scaled_first - unit_share * jnp.mean(scaled_first * unit_share, axis=-1, keepdims=True)
    )

    def joined(*parts):
        return jnp.concatenate(parts, axis=1).astype(f32)

    piece = lambda summed, at: summed[:, at * unit : (at + 1) * unit]
    grad_down = joined(first_sum, piece(third_sum, 0), piece(ring_sum, 0), piece(fourth_sum, 0)).T
    grad_gate = joined(
        piece(second_sum, 0), piece(third_sum, 1), piece(ring_sum, 1), piece(fourth_sum, 1)
    )
    grad_up = joined(
        piece(second_sum, 1), piece(third_sum, 2), piece(ring_sum, 2), piece(fourth_sum, 2)
    )
    query_end = query_cols
    key_end = query_end + kv_cols
    value_end = key_end + kv_cols
    cut = lambda first, end: last_sum[:, first:end].astype(f32)
    gains_out = cut(total - 128, total - 126)
    return (
        block_out,
        input_grad,
        gains_out[:, 0],
        cut(0, query_end),
        cut(query_end, key_end),
        cut(key_end, value_end),
        cut(value_end, total - 128).T,
        gains_out[:, 1],
        grad_gate,
        grad_up,
        grad_down,
    )


def solution(mesh):
    in_specs = (
        P("dp", "ctx", None),
        P(),
        P(None, "tensor"),
        P(None, "tensor"),
        P(None, "tensor"),
        P("tensor", None),
        P(),
        P(None, "tensor"),
        P(None, "tensor"),
        P("tensor", None),
        P("dp", "ctx", None),
    )
    out_specs = (
        P("dp", ("ctx", "tensor"), None),
        P("dp", ("ctx", "tensor"), None),
        P(("dp", "ctx")),
        P(("dp", "ctx"), "tensor"),
        P(("dp", "ctx"), "tensor"),
        P(("dp", "ctx"), "tensor"),
        P("tensor", ("dp", "ctx")),
        P(("dp", "ctx")),
        P(("dp", "ctx"), "tensor"),
        P(("dp", "ctx"), "tensor"),
        P("tensor", ("dp", "ctx")),
    )

    return jax.shard_map(shards, mesh=mesh, in_specs=in_specs, out_specs=out_specs, check_vma=False)
```
